32 devices in a mesh: rel: 4 (over z), node: 2 (over x), head: 4 (over y, core).
Axes of the slice: x: 2, y: 2, z: 4, core: 2. Of those that a mesh axis runs over, the one named last changes fastest.
Arguments:
- features: bfloat16 [4096, 512], P('node'), may hold values from -26 to 26
- node_type: int32 [4096], P('node'), may hold values from 0 to 3
- w_query: bfloat16 [4, 512, 512], P(None, None, 'head'), may hold values from -0.25 to 0.25
- w_key: bfloat16 [4, 512, 512], P(None, None, 'head'), may hold values from -0.25 to 0.25
- w_value: bfloat16 [4, 512, 512], P(None, None, 'head'), may hold values from -0.25 to 0.25
- rel_att: bfloat16 [64, 8, 64, 64], P(None, 'head'), may hold values from -0.75 to 0.75
- rel_msg: bfloat16 [64, 8, 64, 64], P(None, 'head'), may hold values from -0.75 to 0.75
- rel_prior: float32 [64, 8], P(None, 'head'), may hold values from 0.5 to 3
- w_out: bfloat16 [4, 512, 512], P(None, 'head'), may hold values from -0.25 to 0.25
- skip: float32 [4], replicated, may hold values from -1.5 to 1.5
- rel_perm: int32 [64], P('rel'), may hold values from 0 to 63, each once
- tile_src: int32 [64, 32], P('rel', 'node'), may hold values from 0 to 31
- tile_dst: int32 [64, 32], P('rel', 'node'), may hold values from 0 to 15
- tile_bits: int32 [64, 32, 128, 4], P('rel', 'node'), may hold values from -2147483648 to 2147483646
- tile_count: int32 [64, 2], P('rel', 'node'), may hold values from 1 to 16, as said below
Outputs:
- updated: bfloat16 [4096, 512], P(('node', 'head'))
The draws below stay inside these ranges and needn't reach their ends.
Inputs may be any that keep to these rules, and one draw needn't show every extreme that they name: The first tile_count[p, g] slots of group g of position p are live; the words of the other slots may have bits set, but those bits give no edges and must be ignored. Some position has all 16 slots live in every group.
All inputs are finite; a program needn't handle non-finite values.
Results may differ from the reference program's by a relative error of at most 0.008.
The reference program's roundings to bfloat16 on the way (of `qrel` and `hidden`) count: a program that leaves them out, or rounds other values in their place, can miss the bound.
Values may be sent and summed in bfloat16 or wider, within the bound.
A program may use at most 128 MiB of HBM per device.

```python
import math
import jax
import jax.numpy as jnp
from jax import lax

D = 512
HEADS = 8
TYPES = 4
RELS = 64
BLOCK = 128
NB_DEV = 16
TCAP = 16
HD = 64
WORDS = 4
NSHARD = 2
NBLOCKS = 32
NODES = 4096
TILE_SLOTS = 32


def draw_features(key, part):
    first = jax.random.fold_in(key, 0)
    base = jnp.clip(jax.random.normal(first, (NODES, D), jnp.float32), -6.0, 6.0)
    return base.astype(jnp.bfloat16)


def draw_tile_count(key, part):
    first, second, third = jax.random.split(key, 3)
    lowest = max(TCAP // 10, 1)
    sizes = jax.random.randint(first, (RELS, 1), lowest, TCAP + 1)
    drops = jax.random.randint(second, (RELS, NSHARD), 0, 4)
    counts = sizes - drops * sizes // 8
    chosen = jax.random.randint(third, (), 0, RELS)
    rows = jnp.arange(RELS, dtype=jnp.int32)[:, None]
    counts = jnp.where(rows == chosen, TCAP, counts)
    return jnp.maximum(counts, 1).astype(jnp.int32)


def slot_targets(key):
    return jax.random.randint(jax.random.fold_in(key, 11), (RELS, TILE_SLOTS), 0, NB_DEV).astype(jnp.int32)


def draw_tile_dst(key, part):
    return slot_targets(key)


def draw_tile_bits(key, part):
    targets = slot_targets(key)
    packed = jax.random.randint(jax.random.fold_in(key, 13), (RELS, TILE_SLOTS, BLOCK, WORDS), -2147483648, 2147483647, dtype=jnp.int32)
    marked = jax.random.randint(jax.random.fold_in(key, 17), (NBLOCKS, BLOCK), 0, 16)
    chosen = jax.random.randint(jax.random.fold_in(key, 19), (), 0, NBLOCKS * BLOCK)
    node_ids = jnp.arange(NBLOCKS * BLOCK, dtype=jnp.int32).reshape(NBLOCKS, BLOCK)
    lonely = (marked == 0) | (node_ids == chosen)
    groups = jnp.arange(TILE_SLOTS, dtype=jnp.int32) // TCAP
    blocks = (groups[None, :] * NB_DEV + targets).astype(jnp.int32)
    silenced = lonely[blocks]
    return jnp.where(silenced[..., None], 0, packed).astype(jnp.int32)


def with_ends(result, own_key, smallest, top_value):
    longest = result.shape.index(max(result.shape))
    spots = []
    for shift in (0, 1):
        where = [jax.random.randint(jax.random.fold_in(own_key, axis), (), 0, length) for axis, length in enumerate(result.shape)]
        where[longest] = (where[longest] + shift) % result.shape[longest]
        spots.append(tuple(where))
    return result.at[spots[0]].set(smallest).at[spots[1]].set(top_value)


def steps_of(rng, shape, pieces, low, largest):
    level, own = 1.0, jax.random.fold_in(rng, 6)
    for position, shards_of in pieces:
        draws = jnp.exp(jax.random.uniform(jax.random.fold_in(own, position), (shards_of,), jnp.float32, low / len(pieces), largest / len(pieces)))
        level = level * jnp.repeat(draws, shape[position] // shards_of).reshape([-1 if axis == position else 1 for axis in range(len(shape))])
    return level


def normal_values(stream_key, shape, spread, bound, cuts=(), held_as=jnp.bfloat16):
    factor_of = steps_of(stream_key, shape, cuts, -0.22, 0.18) if cuts else 1.0
    array = jax.random.normal(stream_key, shape, jnp.float32) * spread * factor_of
    return jnp.minimum(jnp.maximum(array, -bound), bound).astype(held_as)


def setup_inputs(seed: int = 0) -> dict:
    seeds = jax.random.split(jax.random.key(seed), 16)
    return {
        "features": draw_features(jax.random.fold_in(seeds[15], 71), 0),
        "node_type": with_ends(jax.random.randint(seeds[1], (NODES,), 0, TYPES), jax.random.fold_in(seeds[1], 1), 0, TYPES - 1).astype(jnp.int32),
        "w_query": normal_values(seeds[2], (TYPES, D, D), D ** -0.5, 0.25, ((2, 4),)),
        "w_key": normal_values(seeds[3], (TYPES, D, D), D ** -0.5, 0.25, ((2, 4),)),
        "w_value": normal_values(seeds[4], (TYPES, D, D), D ** -0.5, 0.25, ((2, 4),)),
        "rel_att": normal_values(seeds[5], (RELS, HEADS, HD, HD), HD ** -0.5, 0.75, ((1, 4),)),
        "rel_msg": normal_values(seeds[6], (RELS, HEADS, HD, HD), HD ** -0.5, 0.75, ((1, 4),)),
        "rel_prior": jnp.clip(jnp.exp(math.log(3.0) - 1.7917595 * jax.random.uniform(seeds[7], (RELS, HEADS), jnp.float32) ** steps_of(seeds[7], (RELS, HEADS), ((1, 4),), -0.2, 0.2)), 0.5, 3.0),
        "w_out": normal_values(seeds[8], (TYPES, D, D), D ** -0.5, 0.25, ((1, 4),)),
        "skip": jnp.clip(jax.random.uniform(seeds[9], (TYPES,), jnp.float32, -1.5, 1.5), -1.5, 1.5),
        "rel_perm": jax.random.permutation(seeds[10], RELS).astype(jnp.int32),
        "tile_src": with_ends(jax.random.randint(seeds[11], (RELS, TILE_SLOTS), 0, NBLOCKS), jax.random.fold_in(seeds[11], 1), 0, NBLOCKS - 1).astype(jnp.int32),
        "tile_dst": draw_tile_dst(jax.random.fold_in(seeds[15], 71), 0),
        "tile_bits": draw_tile_bits(jax.random.fold_in(seeds[15], 71), 0),
        "tile_count": draw_tile_count(jax.random.fold_in(seeds[15], 71), 0),
    }


NEG = -1e+30

def project(rows, types, weights):
    total = jnp.zeros((rows.shape[0], weights.shape[2]), jnp.float32)
    for kind in range(weights.shape[0]):
        partial_out = jnp.dot(rows, weights[kind], preferred_element_type=jnp.float32)
        total = jnp.where((types == kind)[:, None], partial_out, total)
    return total

def unpack(words):
    shifts = jnp.arange(32, dtype=jnp.int32)
    bits = words[..., None] >> shifts & 1
    return bits.reshape(words.shape[:-1] + (words.shape[-1] * 32,)) > 0

def reference(features, node_type, w_query, w_key, w_value, rel_att, rel_msg, rel_prior, w_out, skip, rel_perm, tile_src, tile_dst, tile_bits, tile_count):
    query = project(features, node_type, w_query).astype(jnp.bfloat16)
    key = project(features, node_type, w_key).astype(jnp.bfloat16)
    value = project(features, node_type, w_value).astype(jnp.bfloat16)
    query_f = query.reshape(NODES, HEADS, HD).astype(jnp.float32)
    key_blocks = key.reshape(NBLOCKS, BLOCK, HEADS, HD)
    value_blocks = value.reshape(NBLOCKS, BLOCK, HEADS, HD)
    factor = 1.0 / math.sqrt(HD)
    slot_ids = jnp.arange(TILE_SLOTS, dtype=jnp.int32)
    shard = slot_ids // TCAP

    def visit(carry, item):
        m_run, l_run, acc = carry
        relation, src, dst_local, words, counts = item
        live = slot_ids % TCAP < counts[shard]
        dst = (shard * NB_DEV + dst_local).astype(jnp.int32)
        att = rel_att[relation].astype(jnp.float32)
        msg_w = rel_msg[relation].astype(jnp.float32)
        prior = rel_prior[relation] * factor
        qrel = (jnp.einsum('nhe,hde->nhd', query_f, att) * prior[None, :, None]).astype(jnp.bfloat16)
        qrel = qrel.reshape(NBLOCKS, BLOCK, HEADS, HD)
        q_t = qrel[dst].astype(jnp.float32)
        k_t = key_blocks[src].astype(jnp.float32)
        v_t = value_blocks[src].astype(jnp.float32)
        message = jnp.einsum('sjhd,hde->sjhe', v_t, msg_w).astype(jnp.bfloat16)
        scores = jnp.einsum('sihd,sjhd->shij', q_t, k_t)
        edges = unpack(words) & live[:, None, None]
        masked = jnp.where(edges[:, None], scores, NEG)
        block_top = jax.ops.segment_max(masked.max(-1), dst, num_segments=NBLOCKS)
        m_new = jnp.maximum(m_run, block_top)
        weights = jnp.where(edges[:, None], jnp.exp(masked - m_new[dst][..., None]), 0.0)
        rescale = jnp.exp(m_run - m_new)
        l_new = l_run * rescale + jax.ops.segment_sum(weights.sum(-1), dst, num_segments=NBLOCKS)
        pv = jnp.einsum('shij,sjhe->sihe', weights.astype(jnp.bfloat16).astype(jnp.float32), message.astype(jnp.float32))
        acc_new = acc * rescale.transpose(0, 2, 1)[..., None] + jax.ops.segment_sum(pv, dst, num_segments=NBLOCKS)
        return ((m_new, l_new, acc_new), None)
    init = (jnp.full((NBLOCKS, HEADS, BLOCK), NEG, jnp.float32), jnp.zeros((NBLOCKS, HEADS, BLOCK), jnp.float32), jnp.zeros((NBLOCKS, BLOCK, HEADS, HD), jnp.float32))
    (m_run, l_run, acc), _ = lax.scan(visit, init, (rel_perm, tile_src, tile_dst, tile_bits, tile_count))
    totals = l_run.transpose(0, 2, 1).reshape(NODES, HEADS)
    agg = acc.reshape(NODES, D) / jnp.repeat(jnp.maximum(totals, 1.0), HD, axis=1)
    hidden = jax.nn.gelu(agg).astype(jnp.bfloat16)
    mixed = project(hidden, node_type, w_out)
    gate = jax.nn.sigmoid(skip)[node_type][:, None]
    return (gate * mixed + (1.0 - gate) * features.astype(jnp.float32)).astype(jnp.bfloat16)
```

```python
import functools
import math

import jax
import jax.numpy as jnp
from jax import lax
from jax.experimental import pallas as pl
from jax.experimental.pallas import tpu as pltpu
from jax.sharding import PartitionSpec as P

NEG = -1e30
FLOOR = -1e29
GROUP = 4
CHUNK = 4
PAD_ROWS = 16
VMEM_BYTES = 30 * 1024 * 1024


def column(types_row):
    size = types_row.shape[1]
    return jnp.broadcast_to(types_row.astype(jnp.float32), (size, size)).T


def bits_for(count):
    return max(int(count - 1).bit_length(), 1)


def own_block(local, per, n_rel, r):
    return (local // per) * per * n_rel + r * per + local % per


def project_rows(x, weights):
    return [jnp.dot(x, w, preferred_element_type=jnp.float32) for w in weights]


def compact(meta, own_blocks, per, n_rel, r, fields, list_ref):
    src_bits, dst_bits, slot_bits, rel_bits, own_bits = fields
    rows, lanes = meta.shape
    live = meta >= 0
    src = meta & ((1 << src_bits) - 1)
    dst = lax.shift_right_logical(meta, src_bits) & ((1 << dst_bits) - 1)
    rel = lax.shift_right_logical(meta, src_bits + dst_bits) & ((1 << rel_bits) - 1)
    slot = lax.broadcasted_iota(jnp.int32, meta.shape, 0) * lanes + lax.broadcasted_iota(jnp.int32, meta.shape, 1)
    base = slot | lax.shift_left(src, slot_bits) | lax.shift_left(rel, slot_bits + src_bits)
    top = slot_bits + src_bits + rel_bits
    base = base | (1 << (top + own_bits))
    bf = jnp.bfloat16
    hits = [live & (dst == own_block(d, per, n_rel, r)) for d in range(own_blocks)]
    flags = jnp.concatenate([jnp.where(hit, 1.0, 0.0) for hit in hits], axis=0).astype(bf)
    size = own_blocks * rows
    before = lax.broadcasted_iota(jnp.int32, (lanes, lanes), 0) < lax.broadcasted_iota(jnp.int32, (lanes, lanes), 1)
    in_row = jnp.dot(flags, jnp.where(before, 1.0, 0.0).astype(bf), preferred_element_type=jnp.float32)
    row_sum = jnp.dot(flags, jnp.ones((lanes, lanes), bf), preferred_element_type=jnp.float32).astype(bf)
    i = lax.broadcasted_iota(jnp.int32, (size, size), 0)
    j = lax.broadcasted_iota(jnp.int32, (size, size), 1)
    same = jnp.zeros((size, size), jnp.bool_)
    for d in range(own_blocks):
        lo, hi = d * rows, (d + 1) * rows
        same = same | ((i >= lo) & (i < hi) & (j >= lo) & (j < hi))
    ahead = jnp.where(same & (j < i), 1.0, 0.0).astype(bf)
    both = jnp.where(same, 1.0, 0.0).astype(bf)
    rows_before = jnp.dot(ahead, row_sum, preferred_element_type=jnp.float32)
    totals = jnp.dot(both, row_sum, preferred_element_type=jnp.float32)
    rank = jnp.full(meta.shape, -1.0, jnp.float32)
    entry = base
    start = jnp.zeros(meta.shape, jnp.float32)
    for d in range(own_blocks):
        part = slice(d * rows, (d + 1) * rows)
        place = start + rows_before[part] + in_row[part]
        rank = jnp.where(hits[d], place, rank)
        entry = jnp.where(hits[d], base | (d << top), entry)
        start = start + jnp.floor((totals[part] + (GROUP - 1)) * (1.0 / GROUP)) * GROUP
    pieces = [(lax.shift_right_logical(entry, 8 * q) & 255).astype(jnp.float32) for q in range(4)]
    row_entries = []
    for a in range(rows):
        parts = [piece[a : a + 1] for piece in pieces] + [jnp.zeros((4, lanes), jnp.float32)]
        row_entries.append(jnp.concatenate(parts, axis=0).astype(bf))
    places = lax.broadcasted_iota(jnp.int32, (lanes, lanes), 0).astype(jnp.float32)
    for k in range(list_ref.shape[0] - 1):
        ids = places + float(k * lanes)
        found = jnp.zeros((8, lanes), jnp.float32)
        for a in range(rows):
            hot = jnp.where(ids == rank[a : a + 1], 1.0, 0.0).astype(bf)
            found = found + lax.dot_general(
                row_entries[a], hot, (((1,), (1,)), ((), ())), preferred_element_type=jnp.float32
            )
        whole = found.astype(jnp.int32)
        line = whole[0:1]
        for q in range(1, 4):
            line = line | lax.shift_left(whole[q : q + 1], 8 * q)
        list_ref[k : k + 1] = line
    groups = (start[0:1] * (1.0 / GROUP)).astype(jnp.int32)
    list_ref[list_ref.shape[0] - 1 :] = groups


def prepare_kernel(n_rel, n_node, n_head, fields, *refs):
    (packed_ref, types_ref, feat_ref, wk_ref, wv_ref, wq_ref, att_ref, msg_ref, wout_ref, bits_ref) = refs[:10]
    (k_all, vt_all, qt_ref, att_out, msg_out, bits_all, w_all, list_ref) = refs[10:18]
    (x_v, wk_v, wv_v, wq_v, att_v, msg_v, meta_all) = refs[18:25]
    (local, z_send, z_recv, y_send, y_recv, d_send, d_recv, m_send, m_recv, x_send, x_recv, o_send, o_recv) = refs[25:]
    blocks = types_ref.shape[0]
    block = types_ref.shape[1]
    cols = wk_v.shape[2]
    kinds = wk_v.shape[0]
    slots = bits_ref.shape[0]
    share = slots // n_head
    own_blocks = qt_ref.shape[0]
    per = own_blocks // n_head
    chunks = blocks // CHUNK
    rows = CHUNK * block
    relations, heads, size = att_v.shape[0], att_v.shape[1], att_v.shape[2]
    r = lax.axis_index("rel")
    n = lax.axis_index("node")
    h = lax.axis_index("head")
    sibling = h + 1 - 2 * lax.rem(h, 2)
    pairs = list(range(2, n_head, 2))
    bf = jnp.bfloat16

    def fetch(src, dst, index):
        copy = pltpu.make_async_copy(src, dst, local.at[index])
        copy.start()
        return copy

    own_bits = fetch(bits_ref, bits_all.at[pl.ds(pl.multiple_of(r * slots, slots), slots)], 0)
    got_w = [fetch(wk_ref, wk_v, 1), fetch(wv_ref, wv_v, 2)]
    got_x = []
    for c in range(chunks):
        got_x.append(fetch(feat_ref.at[pl.ds(c * rows, rows)], x_v.at[pl.ds(c * rows, rows)], 8 + c))
    got_q = fetch(wq_ref, wq_v, 3)
    got_rel = [fetch(att_ref, att_v, 4), fetch(msg_ref, msg_v, 5)]
    got_out = fetch(wout_ref, w_all.at[h], 6)

    barrier = pltpu.get_barrier_semaphore()
    for t in range(1, n_rel):
        pl.semaphore_signal(barrier, inc=1, device_id={"rel": lax.rem(r + t, n_rel)})
    for t in range(1, n_node):
        pl.semaphore_signal(barrier, inc=1, device_id={"node": lax.rem(n + t, n_node)})
    for t in pairs:
        pl.semaphore_signal(barrier, inc=1, device_id={"head": lax.rem(h + t, n_head)})
    pl.semaphore_signal(barrier, inc=1, device_id={"head": sibling})
    meta_all[pl.ds(r, 1)] = packed_ref[...].reshape((1,) + packed_ref.shape)
    pl.semaphore_wait(barrier, n_rel - 1 + n_node - 1 + len(pairs) + 1)

    started = []

    def send(src, dst, send_sem, recv_sem, target):
        copy = pltpu.make_async_remote_copy(
            src_ref=src, dst_ref=dst, send_sem=send_sem, recv_sem=recv_sem, device_id=target
        )
        copy.start()
        started.append(copy)
        return copy

    def bit_rows(rel, head):
        return bits_all.at[pl.ds(pl.multiple_of(rel * slots + head * share, share), share)]

    own_bits.wait()
    metas, zs = [], []
    for t in range(1, n_rel):
        target = {"rel": lax.rem(r + t, n_rel)}
        metas.append(send(meta_all.at[r], meta_all.at[r], m_send.at[t], m_recv.at[t], target))
    for t in range(1, n_rel):
        target = {"rel": lax.rem(r + t, n_rel)}
        zs.append(send(bit_rows(r, h), bit_rows(r, h), z_send.at[t], z_recv.at[t], target))

    for copy in got_w:
        copy.wait()
    xs = []
    for c in range(chunks):
        got_x[c].wait()
        x = x_v[c * rows : (c + 1) * rows]
        masks = [column(types_ref[c * CHUNK + b : c * CHUNK + b + 1, :]) for b in range(CHUNK)]
        totals = [None] * CHUNK
        for kind in range(kinds):
            both = jnp.concatenate([wk_v[kind], wv_v[kind]], axis=1)
            out = jnp.dot(x, both, preferred_element_type=jnp.float32)
            for b in range(CHUNK):
                piece = out[b * block : (b + 1) * block]
                pair = (piece[:, :cols], piece[:, cols:])
                if totals[b] is None:
                    totals[b] = pair
                else:
                    hit = masks[b] == float(kind)
                    totals[b] = tuple(jnp.where(hit, new, old) for new, old in zip(pair, totals[b]))
        first = n * blocks + c * CHUNK
        for b in range(CHUNK):
            k_all[first + b] = totals[b][0].astype(bf)
            vt_all[first + b] = totals[b][1].T.astype(bf)
        for t in range(1, n_node):
            target = {"node": lax.rem(n + t, n_node)}
            for which, ref in enumerate((k_all, vt_all)):
                part = ref.at[pl.ds(first, CHUNK)]
                xs.append(send(part, part, x_send.at[t, c, which], x_recv.at[t, c, which], target))

    got_q.wait()
    wide = jnp.concatenate([wq_v[kind] for kind in range(kinds)], axis=1)
    mine = [own_block(d, per, n_rel, r) for d in range(own_blocks)]
    x = jnp.concatenate([x_v[pl.ds(pl.multiple_of(b * block, block), block)] for b in mine], axis=0)
    out = jnp.dot(x, wide, preferred_element_type=jnp.float32)
    for d in range(own_blocks):
        mask = column(types_ref[pl.ds(mine[d], 1), :])
        piece = out[d * block : (d + 1) * block]
        total = piece[:, :cols]
        for kind in range(1, kinds):
            total = jnp.where(mask == float(kind), piece[:, kind * cols : (kind + 1) * cols], total)
        qt_ref[d] = total.T.astype(bf)

    got_out.wait()
    os = []
    for i, t in enumerate(pairs):
        target = {"head": lax.rem(h + t, n_head)}
        os.append(send(w_all.at[h], w_all.at[h], o_send.at[i], o_recv.at[i], target))
    own_out = send(w_all.at[h], w_all.at[h], o_send.at[len(pairs)], o_recv.at[len(pairs)], {"head": sibling})

    def diagonal(ref, index):
        lines = []
        for k in range(heads):
            parts = [jnp.zeros((size, size), jnp.float32)] * heads
            parts[k] = ref[index, k].astype(jnp.float32)
            lines.append(jnp.concatenate(parts, axis=1))
        return jnp.concatenate(lines, axis=0)

    def relation(index, carry):
        att_out[index] = diagonal(att_v, index).astype(bf)
        msg_out[index] = diagonal(msg_v, index).T.astype(bf)
        return carry

    for copy in got_rel:
        copy.wait()
    ys, ds = [], []
    step = relations // n_rel
    for t in range(1, n_rel):
        lax.fori_loop((t - 1) * step, relations if t == n_rel - 1 else t * step, relation, 0)
        zs[t - 1].wait_recv()
        source = lax.rem(r + n_rel - t, n_rel)
        for i, u in enumerate(pairs):
            target = {"head": lax.rem(h + u, n_head)}
            ys.append((t, u, send(bit_rows(source, h), bit_rows(source, h), y_send.at[t, i], y_recv.at[t, i], target)))
        ds.append(
            send(bit_rows(source, h), bit_rows(source, h), d_send.at[t, 0], d_recv.at[t, 0], {"head": sibling})
        )

    for copy in metas:
        copy.wait_recv()
    used = slots // block
    meta = jnp.concatenate([meta_all[s, :used] for s in range(n_rel)], axis=0)
    compact(meta, own_blocks, per, n_rel, r, fields, list_ref)

    for i, (t, u, copy) in enumerate(ys):
        copy.wait_recv()
        source = lax.rem(r + n_rel - t, n_rel)
        head = lax.rem(h + n_head - u, n_head)
        which = 1 + pairs.index(u)
        ds.append(
            send(bit_rows(source, head), bit_rows(source, head), d_send.at[t, which], d_recv.at[t, which], {"head": sibling})
        )
    for i, t in enumerate(pairs):
        os[i].wait_recv()
        head = lax.rem(h + n_head - t, n_head)
        index = len(pairs) + 1 + i
        ds.append(send(w_all.at[head], w_all.at[head], o_send.at[index], o_recv.at[index], {"head": sibling}))
    own_out.wait_recv()
    for copy in ds:
        copy.wait_recv()
    for copy in xs:
        copy.wait_recv()
    for copy in started:
        copy.wait_send()


def tile_kernel(heads, factor, fields, list_ref, prior_ref, qt_ref, k_ref, vt_ref, bits_ref, att_ref, msg_ref, *refs):
    acc_ref, top_ref, left, right, scores, peak = refs
    src_bits, _, slot_bits, rel_bits, own_bits = fields
    own_blocks, cols, block = qt_ref.shape
    size = cols // heads
    words = bits_ref.shape[1]
    tall = acc_ref.shape[1]
    span = heads * block
    groups = list_ref[list_ref.shape[0] - 1, 0]

    acc_ref[...] = jnp.zeros_like(acc_ref)
    top_ref[...] = jnp.full_like(top_ref, FLOOR)
    right[...] = jnp.zeros_like(right)
    row = lax.broadcasted_iota(jnp.int32, (tall, span), 0)
    lane = lax.broadcasted_iota(jnp.int32, (tall, span), 1)
    ones = jnp.zeros((tall, span), jnp.float32)
    for k in range(heads):
        ones = jnp.where((row == cols + k) & (lane >= k * block) & (lane < (k + 1) * block), 1.0, ones)
    ones = ones.astype(jnp.bfloat16)
    for u in range(GROUP):
        left[:, u * span : (u + 1) * span] = ones
    bit_of = lax.shift_left(jnp.int32(1), lax.broadcasted_iota(jnp.int32, (32, block), 0))
    sum_row = lax.broadcasted_iota(jnp.int32, (tall - cols, block), 0)

    def entries(group):
        line = lax.shift_right_logical(group * GROUP, 7)
        start = (group * GROUP) & 127
        found = []
        for u in range(GROUP):
            value = list_ref[line, start + u]
            slot = value & ((1 << slot_bits) - 1)
            rest = lax.shift_right_logical(value, slot_bits)
            src = rest & ((1 << src_bits) - 1)
            rest = lax.shift_right_logical(rest, src_bits)
            rel = rest & ((1 << rel_bits) - 1)
            rest = lax.shift_right_logical(rest, rel_bits)
            dst = rest & ((1 << own_bits) - 1)
            valid = -lax.shift_right_logical(rest, own_bits)
            found.append((slot, src, rel, dst, valid))
        return found

    def turn(group):
        picks = entries(group)
        dst = picks[0][3]
        stack = jnp.concatenate([att_ref[rel] for _, _, rel, _, _ in picks], axis=0)
        turned = jnp.dot(stack, qt_ref[dst], preferred_element_type=jnp.float32)
        for u, (_, _, rel, _, _) in enumerate(picks):
            for k in range(heads):
                lo = u * cols + k * size
                scaled = turned[lo : lo + size] * (prior_ref[rel * heads + k] * factor)
                right[u, k * size : (k + 1) * size, k * block : (k + 1) * block] = scaled.astype(jnp.bfloat16)

    def send_messages(group):
        for u, (_, src, rel, _, _) in enumerate(entries(group)):
            message = jnp.dot(msg_ref[rel], vt_ref[src], preferred_element_type=jnp.float32).astype(jnp.bfloat16)
            for k in range(heads):
                lo = u * span + k * block
                left[k * size : (k + 1) * size, lo : lo + block] = message[k * size : (k + 1) * size]

    def score(group):
        best = [None] * heads
        for u, (slot, src, _, _, valid) in enumerate(entries(group)):
            found = jnp.dot(k_ref[src], right[u], preferred_element_type=jnp.float32)
            tile_words = bits_ref[slot] & valid
            edges = jnp.concatenate([(tile_words[w : w + 1] & bit_of) != 0 for w in range(words)], axis=0)
            for k in range(heads):
                masked = jnp.where(edges, found[:, k * block : (k + 1) * block], NEG)
                scores[u * heads + k] = masked
                top = jnp.max(masked.reshape(block // 8, 8, block), axis=0)
                best[k] = top if best[k] is None else jnp.maximum(best[k], top)
        for k in range(heads):
            peak[k : k + 1] = jnp.max(best[k], axis=0, keepdims=True)

    def gather(group):
        dst = entries(group)[0][3]
        keeps, weights = [], [None] * (GROUP * heads)
        for k in range(heads):
            old = top_ref[dst, k : k + 1]
            new = jnp.maximum(old, peak[k : k + 1])
            top_ref[dst, k : k + 1] = new
            keeps.append(jnp.exp(old - new))
            for u in range(GROUP):
                weights[u * heads + k] = jnp.exp(scores[u * heads + k] - new).astype(jnp.bfloat16)
        out = jnp.dot(left[...], jnp.concatenate(weights, axis=0), preferred_element_type=jnp.float32)
        for k in range(heads):
            rows = slice(k * size, (k + 1) * size)
            acc_ref[dst, rows] = acc_ref[dst, rows] * keeps[k] + out[rows]
        keep = jnp.broadcast_to(keeps[0], sum_row.shape)
        for k in range(1, heads):
            keep = jnp.where(sum_row == k, keeps[k], keep)
        acc_ref[dst, cols:] = acc_ref[dst, cols:] * keep + out[cols:]

    def visit(group, carry):
        gather(group)
        score(group + 1)
        send_messages(group + 1)
        turn(group + 2)
        return carry

    turn(0)
    score(0)
    send_messages(0)
    turn(1)
    lax.fori_loop(0, groups, visit, 0)


def finish_kernel(n_rel, n_head, heads, acc_ref, types_ref, skip_ref, feat_ref, w_ref, *refs):
    out_ref, hid_out, hid_got, resid, send_sem, recv_sem, local = refs
    own_blocks, _, block = acc_ref.shape
    kinds = w_ref.shape[1]
    cols = w_ref.shape[2]
    width = w_ref.shape[3]
    size = cols // heads
    per = own_blocks // n_head
    piece = per * block
    r = lax.axis_index("rel")
    h = lax.axis_index("head")
    span = n_rel * piece

    fetch = pltpu.make_async_copy(feat_ref.at[pl.ds(pl.multiple_of(h * span, span), span)], resid, local.at[0])
    fetch.start()
    barrier = pltpu.get_barrier_semaphore()
    shifts = [(a, b) for b in range(n_head) for a in range(n_rel) if a or b]
    for a, b in shifts:
        target = {"rel": lax.rem(r + a, n_rel), "head": lax.rem(h + b, n_head)}
        pl.semaphore_signal(barrier, inc=1, device_id=target)

    def hidden_of(source):
        total = jnp.maximum(acc_ref[source, cols : cols + 8], 1.0)
        sides = []
        for k in range(heads):
            sides.append(acc_ref[source, pl.ds(k * size, size)] / total[k : k + 1])
        agg = jnp.concatenate(sides, axis=0)
        inner = math.sqrt(2.0 / math.pi) * (agg + 0.044715 * (agg * agg * agg))
        hidden = agg * (0.5 * (1.0 + jnp.tanh(inner)))
        return hidden.T.astype(jnp.bfloat16)

    for b in range(n_head):
        head = lax.rem(h + b, n_head)
        for i in range(per):
            hid_out[b, i * block : (i + 1) * block] = hidden_of(head * per + i)
    pl.semaphore_wait(barrier, len(shifts))

    sends = {}
    for a, b in sorted(shifts, key=lambda s: (s[0] == 0, s[1])):
        target = {"rel": lax.rem(r + a, n_rel), "head": lax.rem(h + b, n_head)}
        copy = pltpu.make_async_remote_copy(
            src_ref=hid_out.at[b],
            dst_ref=hid_got.at[a, b],
            send_sem=send_sem.at[a, b],
            recv_sem=recv_sem.at[a, b],
            device_id=target,
        )
        copy.start()
        sends[a, b] = copy
    hid_got[0, 0] = hid_out[0]
    fetch.wait()
    gates = []
    for a in range(n_rel):
        source = lax.rem(r + n_rel - a, n_rel)
        for b in range(n_head):
            if a or b:
                sends[a, b].wait_recv()
        parts = [hid_got[a, lax.rem(h + n_head - head, n_head)] for head in range(n_head)]
        hidden = jnp.concatenate(parts, axis=1)
        outs = []
        for kind in range(kinds):
            weights = jnp.concatenate([w_ref[head, kind] for head in range(n_head)], axis=0)
            outs.append(jnp.dot(hidden, weights, preferred_element_type=jnp.float32))
        for i in range(per):
            mask = column(types_ref[pl.ds((h * n_rel + source) * per + i, 1), :])
            masks = [mask == float(kind) for kind in range(kinds)]
            logit = jnp.full((block, block), skip_ref[0], jnp.float32)
            for kind in range(1, kinds):
                logit = jnp.where(masks[kind], skip_ref[kind], logit)
            gate = 1.0 / (1.0 + jnp.exp(-logit))
            rows = pl.ds(pl.multiple_of(source * piece + i * block, block), block)
            for w in range(width // block):
                lanes = slice(w * block, (w + 1) * block)
                total = outs[0][i * block : (i + 1) * block, lanes]
                for kind in range(1, kinds):
                    total = jnp.where(masks[kind], outs[kind][i * block : (i + 1) * block, lanes], total)
                old = resid[rows, lanes].astype(jnp.float32)
                out_ref[rows, lanes] = (gate * total + (1.0 - gate) * old).astype(jnp.bfloat16)
    for copy in sends.values():
        copy.wait_send()


def per_device(
    features,
    node_type,
    w_query,
    w_key,
    w_value,
    rel_att,
    rel_msg,
    rel_prior,
    w_out,
    skip,
    rel_perm,
    tile_src,
    tile_dst,
    tile_bits,
    tile_count,
):
    node_rows, width = features.shape
    n_rel = lax.axis_size("rel")
    n_node = lax.axis_size("node")
    n_head = lax.axis_size("head")
    relations, heads = rel_prior.shape
    cols = w_query.shape[2]
    kinds = w_query.shape[0]
    block = tile_bits.shape[2]
    words = tile_bits.shape[3]
    blocks = node_rows // block
    positions, tcap = tile_src.shape
    slots = positions * tcap
    factor = 1.0 / math.sqrt(cols // heads)
    own_blocks = blocks // n_rel
    all_slots = n_rel * slots
    bf = jnp.bfloat16
    fields = (
        bits_for(n_node * blocks),
        bits_for(blocks),
        bits_for(all_slots),
        bits_for(relations),
        bits_for(own_blocks),
    )

    live = jnp.arange(tcap, dtype=jnp.int32)[None, :] < tile_count.reshape(positions, 1)
    packed = tile_src | (tile_dst << fields[0]) | (rel_perm[:, None] << (fields[0] + fields[1]))
    packed = jnp.where(live, packed, -1).reshape(slots // block, block)
    packed = jnp.pad(packed, ((0, 8 - slots // block), (0, 0)), constant_values=-1)
    bits = tile_bits.transpose(0, 1, 3, 2).reshape(slots, words, block)

    list_rows = -(-(all_slots + own_blocks * GROUP + 3 * GROUP) // block) + 1
    chunks = blocks // CHUNK
    half = max(n_head // 2 - 1, 1)
    dma = pltpu.SemaphoreType.DMA
    smem = pl.BlockSpec(memory_space=pltpu.SMEM)
    vmem = pl.BlockSpec(memory_space=pltpu.VMEM)
    hbm = pl.BlockSpec(memory_space=pl.ANY)
    shape = jax.ShapeDtypeStruct
    keys, values_t, query_t, att, msg, all_bits, all_out, listed = pl.pallas_call(
        functools.partial(prepare_kernel, n_rel, n_node, n_head, fields),
        in_specs=[vmem, vmem] + [hbm] * 8,
        out_specs=[vmem] * 8,
        out_shape=[
            shape((n_node * blocks, block, cols), bf),
            shape((n_node * blocks, cols, block), bf),
            shape((own_blocks, cols, block), bf),
            shape((relations, cols, cols), bf),
            shape((relations, cols, cols), bf),
            shape((all_slots, words, block), jnp.int32),
            shape((n_head,) + w_out.shape, bf),
            shape((list_rows, block), jnp.int32),
        ],
        scratch_shapes=[
            pltpu.VMEM(features.shape, bf),
            pltpu.VMEM(w_key.shape, bf),
            pltpu.VMEM(w_value.shape, bf),
            pltpu.VMEM(w_query.shape, bf),
            pltpu.VMEM(rel_att.shape, bf),
            pltpu.VMEM(rel_msg.shape, bf),
            pltpu.VMEM((n_rel, 8, block), jnp.int32),
            dma((8 + chunks,)),
            dma((n_rel,)),
            dma((n_rel,)),
            dma((n_rel, half)),
            dma((n_rel, half)),
            dma((n_rel, 1 + half)),
            dma((n_rel, 1 + half)),
            dma((n_rel,)),
            dma((n_rel,)),
            dma((n_node, chunks, 2)),
            dma((n_node, chunks, 2)),
            dma((n_head,)),
            dma((n_head,)),
        ],
        compiler_params=pltpu.CompilerParams(collective_id=0, has_side_effects=True, vmem_limit_bytes=VMEM_BYTES),
        name="prepare",
    )(packed, node_type.reshape(blocks, block), features, w_key, w_value, w_query, rel_att, rel_msg, w_out, bits)

    tall = cols + PAD_ROWS
    acc = pl.pallas_call(
        functools.partial(tile_kernel, heads, factor, fields),
        in_specs=[smem] * 2 + [vmem] * 6,
        out_specs=vmem,
        out_shape=shape((own_blocks, tall, block), jnp.float32),
        scratch_shapes=[
            pltpu.VMEM((own_blocks, 8, block), jnp.float32),
            pltpu.VMEM((tall, GROUP * heads * block), bf),
            pltpu.VMEM((GROUP, cols, heads * block), bf),
            pltpu.VMEM((GROUP * heads, block, block), jnp.float32),
            pltpu.VMEM((8, block), jnp.float32),
        ],
        compiler_params=pltpu.CompilerParams(vmem_limit_bytes=VMEM_BYTES),
        name="tiles",
    )(listed, rel_prior.reshape(-1), query_t, keys, values_t, all_bits, att, msg)

    piece = own_blocks // n_head * block
    return pl.pallas_call(
        functools.partial(finish_kernel, n_rel, n_head, heads),
        in_specs=[vmem, vmem, smem, hbm, vmem],
        out_specs=vmem,
        out_shape=shape((n_rel * piece, width), bf),
        scratch_shapes=[
            pltpu.VMEM((n_head, piece, cols), bf),
            pltpu.VMEM((n_rel, n_head, piece, cols), bf),
            pltpu.VMEM((n_rel * piece, width), bf),
            dma((n_rel, n_head)),
            dma((n_rel, n_head)),
            dma((1,)),
        ],
        compiler_params=pltpu.CompilerParams(collective_id=1, has_side_effects=True, vmem_limit_bytes=VMEM_BYTES),
        name="finish",
    )(acc, node_type.reshape(blocks, block), skip, features, all_out)


def solution(mesh):
    in_specs = (
        P("node", None),
        P("node"),
        P(None, None, "head"),
        P(None, None, "head"),
        P(None, None, "head"),
        P(None, "head", None, None),
        P(None, "head", None, None),
        P(None, "head"),
        P(None, "head", None),
        P(),
        P("rel"),
        P("rel", "node"),
        P("rel", "node"),
        P("rel", "node", None, None),
        P("rel", "node"),
    )
    out_specs = P(("node", "head"), None)
    return jax.shard_map(
        per_device, mesh=mesh, in_specs=in_specs, out_specs=out_specs, check_vma=False
    )
```

```python
import functools
import math

import jax
import jax.numpy as jnp
from jax import lax
from jax.experimental import pallas as pl
from jax.experimental.pallas import tpu as pltpu
from jax.sharding import PartitionSpec as P

NEG = -1e30
FLOOR = -1e29
GROUP = 4
CHUNK = 4
PAD_ROWS = 16
VMEM_BYTES = 30 * 1024 * 1024


def column(types_row):
    size = types_row.shape[1]
    return jnp.broadcast_to(types_row.astype(jnp.float32), (size, size)).T


def in_hbm(value):
    return pltpu.with_memory_space_constraint(value, pltpu.HBM)


def bits_for(count):
    return max(int(count - 1).bit_length(), 1)


def own_block(local, per, n_rel, r):
    return (local // per) * per * n_rel + r * per + local % per


def project_rows(x, weights):
    return [jnp.dot(x, w, preferred_element_type=jnp.float32) for w in weights]


def compact(meta, own_blocks, per, n_rel, r, fields, list_ref):
    src_bits, dst_bits, slot_bits, rel_bits, own_bits = fields
    rows, lanes = meta.shape
    live = meta >= 0
    src = meta & ((1 << src_bits) - 1)
    dst = lax.shift_right_logical(meta, src_bits) & ((1 << dst_bits) - 1)
    rel = lax.shift_right_logical(meta, src_bits + dst_bits) & ((1 << rel_bits) - 1)
    slot = lax.broadcasted_iota(jnp.int32, meta.shape, 0) * lanes + lax.broadcasted_iota(jnp.int32, meta.shape, 1)
    base = slot | lax.shift_left(src, slot_bits) | lax.shift_left(rel, slot_bits + src_bits)
    top = slot_bits + src_bits + rel_bits
    base = base | (1 << (top + own_bits))
    bf = jnp.bfloat16
    hits = [live & (dst == own_block(d, per, n_rel, r)) for d in range(own_blocks)]
    flags = jnp.concatenate([jnp.where(hit, 1.0, 0.0) for hit in hits], axis=0).astype(bf)
    size = own_blocks * rows
    before = lax.broadcasted_iota(jnp.int32, (lanes, lanes), 0) < lax.broadcasted_iota(jnp.int32, (lanes, lanes), 1)
    in_row = jnp.dot(flags, jnp.where(before, 1.0, 0.0).astype(bf), preferred_element_type=jnp.float32)
    row_sum = jnp.dot(flags, jnp.ones((lanes, lanes), bf), preferred_element_type=jnp.float32).astype(bf)
    i = lax.broadcasted_iota(jnp.int32, (size, size), 0)
    j = lax.broadcasted_iota(jnp.int32, (size, size), 1)
    same = jnp.zeros((size, size), jnp.bool_)
    for d in range(own_blocks):
        lo, hi = d * rows, (d + 1) * rows
        same = same | ((i >= lo) & (i < hi) & (j >= lo) & (j < hi))
    ahead = jnp.where(same & (j < i), 1.0, 0.0).astype(bf)
    both = jnp.where(same, 1.0, 0.0).astype(bf)
    rows_before = jnp.dot(ahead, row_sum, preferred_element_type=jnp.float32)
    totals = jnp.dot(both, row_sum, preferred_element_type=jnp.float32)
    rank = jnp.full(meta.shape, -1.0, jnp.float32)
    entry = base
    start = jnp.zeros(meta.shape, jnp.float32)
    for d in range(own_blocks):
        part = slice(d * rows, (d + 1) * rows)
        place = start + rows_before[part] + in_row[part]
        rank = jnp.where(hits[d], place, rank)
        entry = jnp.where(hits[d], base | (d << top), entry)
        start = start + jnp.floor((totals[part] + (GROUP - 1)) * (1.0 / GROUP)) * GROUP
    pieces = [(lax.shift_right_logical(entry, 8 * q) & 255).astype(jnp.float32) for q in range(4)]
    row_entries = []
    for a in range(rows):
        parts = [piece[a : a + 1] for piece in pieces] + [jnp.zeros((4, lanes), jnp.float32)]
        row_entries.append(jnp.concatenate(parts, axis=0).astype(bf))
    places = lax.broadcasted_iota(jnp.int32, (lanes, lanes), 0).astype(jnp.float32)
    for k in range(list_ref.shape[0] - 1):
        ids = places + float(k * lanes)
        found = jnp.zeros((8, lanes), jnp.float32)
        for a in range(rows):
            hot = jnp.where(ids == rank[a : a + 1], 1.0, 0.0).astype(bf)
            found = found + lax.dot_general(
                row_entries[a], hot, (((1,), (1,)), ((), ())), preferred_element_type=jnp.float32
            )
        whole = found.astype(jnp.int32)
        line = whole[0:1]
        for q in range(1, 4):
            line = line | lax.shift_left(whole[q : q + 1], 8 * q)
        list_ref[k : k + 1] = line
    groups = (start[0:1] * (1.0 / GROUP)).astype(jnp.int32)
    list_ref[list_ref.shape[0] - 1 :] = groups


def pack(src, dst, count, perm, fields, lanes):
    positions, tcap = src.shape
    i = lax.broadcasted_iota(jnp.int32, (positions, positions), 0)
    j = lax.broadcasted_iota(jnp.int32, (positions, positions), 1)

    def upright(row):
        return jnp.sum(jnp.where(i == j, row.astype(jnp.float32), 0.0), axis=1, keepdims=True).astype(jnp.int32)

    word = src | lax.shift_left(dst, fields[0]) | lax.shift_left(upright(perm), fields[0] + fields[1])
    slot = lax.broadcasted_iota(jnp.int32, src.shape, 1)
    word = jnp.where(slot < upright(count), word, -1)
    each = lanes // tcap
    rows = [
        jnp.concatenate([word[a + b : a + b + 1] for b in range(each)], axis=1) for a in range(0, positions, each)
    ]
    rows.append(jnp.full((8 - len(rows), lanes), -1, jnp.int32))
    return jnp.concatenate(rows, axis=0).reshape(1, 8, lanes)


def prepare_kernel(n_rel, n_node, n_head, fields, *refs):
    (small, feat_ref, wk_ref, wv_ref, wq_ref, att_ref, msg_ref, wout_ref, bits_ref), refs = (
        (refs[:5],) + refs[5:13],
        refs[13:],
    )
    (k_all, vt_all, qt_ref, att_out, msg_out, bits_all, w_all, list_ref) = refs[:8]
    (x_v, wk_v, wv_v, wq_v, att_v, msg_v, meta_all), refs = refs[8:15], refs[15:]
    (types_ref, src_v, dst_v, count_v, perm_v), refs = refs[:5], refs[5:]
    (local, z_send, z_recv, y_send, y_recv, d_send, d_recv, m_send, m_recv, x_send, x_recv, o_send, o_recv) = refs
    blocks = types_ref.shape[0]
    block = types_ref.shape[1]
    cols = wk_v.shape[2]
    kinds = wk_v.shape[0]
    slots = bits_ref.shape[0]
    share = slots // n_head
    own_blocks = qt_ref.shape[0]
    per = own_blocks // n_head
    chunks = blocks // CHUNK
    rows = CHUNK * block
    relations, heads, size = att_v.shape[0], att_v.shape[1], att_v.shape[2]
    r = lax.axis_index("rel")
    n = lax.axis_index("node")
    h = lax.axis_index("head")
    sibling = h + 1 - 2 * lax.rem(h, 2)
    pairs = list(range(2, n_head, 2))
    bf = jnp.bfloat16

    def fetch(src, dst, index):
        copy = pltpu.make_async_copy(src, dst, local.at[index])
        copy.start()
        return copy

    small_v = (types_ref, src_v, dst_v, count_v, perm_v)
    got_small = [fetch(a, b, 8 + chunks + i) for i, (a, b) in enumerate(zip(small, small_v))]
    own_bits = fetch(bits_ref, bits_all.at[pl.ds(pl.multiple_of(r * slots, slots), slots)], 0)
    got_w = [fetch(wk_ref, wk_v, 1), fetch(wv_ref, wv_v, 2)]
    got_x = []
    for c in range(chunks):
        got_x.append(fetch(feat_ref.at[pl.ds(c * rows, rows)], x_v.at[pl.ds(c * rows, rows)], 8 + c))
    got_q = fetch(wq_ref, wq_v, 3)
    got_rel = [fetch(att_ref, att_v, 4), fetch(msg_ref, msg_v, 5)]
    got_out = fetch(wout_ref, w_all.at[h], 6)

    barrier = pltpu.get_barrier_semaphore()
    for t in range(1, n_rel):
        pl.semaphore_signal(barrier, inc=1, device_id={"rel": lax.rem(r + t, n_rel)})
    for t in range(1, n_node):
        pl.semaphore_signal(barrier, inc=1, device_id={"node": lax.rem(n + t, n_node)})
    for t in pairs:
        pl.semaphore_signal(barrier, inc=1, device_id={"head": lax.rem(h + t, n_head)})
    pl.semaphore_signal(barrier, inc=1, device_id={"head": sibling})
    for copy in got_small:
        copy.wait()
    meta_all[pl.ds(r, 1)] = pack(src_v[...], dst_v[...], count_v[...], perm_v[...], fields, block)
    pl.semaphore_wait(barrier, n_rel - 1 + n_node - 1 + len(pairs) + 1)

    started = []

    def send(src, dst, send_sem, recv_sem, target):
        copy = pltpu.make_async_remote_copy(
            src_ref=src, dst_ref=dst, send_sem=send_sem, recv_sem=recv_sem, device_id=target
        )
        copy.start()
        started.append(copy)
        return copy

    def bit_rows(rel, head):
        return bits_all.at[pl.ds(pl.multiple_of(rel * slots + head * share, share), share)]

    own_bits.wait()
    metas, zs = [], []
    for t in range(1, n_rel):
        target = {"rel": lax.rem(r + t, n_rel)}
        metas.append(send(meta_all.at[r], meta_all.at[r], m_send.at[t], m_recv.at[t], target))
    for t in range(1, n_rel):
        target = {"rel": lax.rem(r + t, n_rel)}
        zs.append(send(bit_rows(r, h), bit_rows(r, h), z_send.at[t], z_recv.at[t], target))

    for copy in got_w:
        copy.wait()
    xs = []
    for c in range(chunks):
        got_x[c].wait()
        x = x_v[c * rows : (c + 1) * rows]
        masks = [column(types_ref[c * CHUNK + b : c * CHUNK + b + 1, :]) for b in range(CHUNK)]
        totals = [None] * CHUNK
        for kind in range(kinds):
            both = jnp.concatenate([wk_v[kind], wv_v[kind]], axis=1)
            out = jnp.dot(x, both, preferred_element_type=jnp.float32)
            for b in range(CHUNK):
                piece = out[b * block : (b + 1) * block]
                pair = (piece[:, :cols], piece[:, cols:])
                if totals[b] is None:
                    totals[b] = pair
                else:
                    hit = masks[b] == float(kind)
                    totals[b] = tuple(jnp.where(hit, new, old) for new, old in zip(pair, totals[b]))
        first = n * blocks + c * CHUNK
        for b in range(CHUNK):
            k_all[first + b] = totals[b][0].astype(bf)
            vt_all[first + b] = totals[b][1].T.astype(bf)
        for t in range(1, n_node):
            target = {"node": lax.rem(n + t, n_node)}
            for which, ref in enumerate((k_all, vt_all)):
                part = ref.at[pl.ds(first, CHUNK)]
                xs.append(send(part, part, x_send.at[t, c, which], x_recv.at[t, c, which], target))

    got_q.wait()
    wide = jnp.concatenate([wq_v[kind] for kind in range(kinds)], axis=1)
    mine = [own_block(d, per, n_rel, r) for d in range(own_blocks)]
    x = jnp.concatenate([x_v[pl.ds(pl.multiple_of(b * block, block), block)] for b in mine], axis=0)
    out = jnp.dot(x, wide, preferred_element_type=jnp.float32)
    for d in range(own_blocks):
        mask = column(types_ref[pl.ds(mine[d], 1), :])
        piece = out[d * block : (d + 1) * block]
        total = piece[:, :cols]
        for kind in range(1, kinds):
            total = jnp.where(mask == float(kind), piece[:, kind * cols : (kind + 1) * cols], total)
        qt_ref[d] = total.T.astype(bf)

    got_out.wait()
    os = []
    for i, t in enumerate(pairs):
        target = {"head": lax.rem(h + t, n_head)}
        os.append(send(w_all.at[h], w_all.at[h], o_send.at[i], o_recv.at[i], target))
    own_out = send(w_all.at[h], w_all.at[h], o_send.at[len(pairs)], o_recv.at[len(pairs)], {"head": sibling})

    def diagonal(ref, index):
        lines = []
        for k in range(heads):
            parts = [jnp.zeros((size, size), jnp.float32)] * heads
            parts[k] = ref[index, k].astype(jnp.float32)
            lines.append(jnp.concatenate(parts, axis=1))
        return jnp.concatenate(lines, axis=0)

    def relation(index, carry):
        att_out[index] = diagonal(att_v, index).astype(bf)
        msg_out[index] = diagonal(msg_v, index).T.astype(bf)
        return carry

    for copy in got_rel:
        copy.wait()
    ys, ds = [], []
    step = relations // n_rel
    for t in range(1, n_rel):
        lax.fori_loop((t - 1) * step, relations if t == n_rel - 1 else t * step, relation, 0)
        zs[t - 1].wait_recv()
        source = lax.rem(r + n_rel - t, n_rel)
        for i, u in enumerate(pairs):
            target = {"head": lax.rem(h + u, n_head)}
            ys.append((t, u, send(bit_rows(source, h), bit_rows(source, h), y_send.at[t, i], y_recv.at[t, i], target)))
        ds.append(
            send(bit_rows(source, h), bit_rows(source, h), d_send.at[t, 0], d_recv.at[t, 0], {"head": sibling})
        )

    for copy in metas:
        copy.wait_recv()
    used = slots // block
    meta = jnp.concatenate([meta_all[s, :used] for s in range(n_rel)], axis=0)
    compact(meta, own_blocks, per, n_rel, r, fields, list_ref)

    for i, (t, u, copy) in enumerate(ys):
        copy.wait_recv()
        source = lax.rem(r + n_rel - t, n_rel)
        head = lax.rem(h + n_head - u, n_head)
        which = 1 + pairs.index(u)
        ds.append(
            send(bit_rows(source, head), bit_rows(source, head), d_send.at[t, which], d_recv.at[t, which], {"head": sibling})
        )
    for i, t in enumerate(pairs):
        os[i].wait_recv()
        head = lax.rem(h + n_head - t, n_head)
        index = len(pairs) + 1 + i
        ds.append(send(w_all.at[head], w_all.at[head], o_send.at[index], o_recv.at[index], {"head": sibling}))
    own_out.wait_recv()
    for copy in ds:
        copy.wait_recv()
    for copy in xs:
        copy.wait_recv()
    for copy in started:
        copy.wait_send()


def tile_kernel(heads, factor, fields, list_ref, prior_ref, qt_ref, k_ref, vt_ref, bits_ref, att_ref, msg_ref, *refs):
    acc_ref, top_ref, left, right, scores, peak = refs
    src_bits, _, slot_bits, rel_bits, own_bits = fields
    own_blocks, cols, block = qt_ref.shape
    size = cols // heads
    words = bits_ref.shape[1]
    tall = acc_ref.shape[1]
    span = heads * block
    groups = list_ref[list_ref.shape[0] - 1, 0]

    acc_ref[...] = jnp.zeros_like(acc_ref)
    top_ref[...] = jnp.full_like(top_ref, FLOOR)
    right[...] = jnp.zeros_like(right)
    row = lax.broadcasted_iota(jnp.int32, (tall, span), 0)
    lane = lax.broadcasted_iota(jnp.int32, (tall, span), 1)
    ones = jnp.zeros((tall, span), jnp.float32)
    for k in range(heads):
        ones = jnp.where((row == cols + k) & (lane >= k * block) & (lane < (k + 1) * block), 1.0, ones)
    ones = ones.astype(jnp.bfloat16)
    for u in range(GROUP):
        left[:, u * span : (u + 1) * span] = ones
    bit_of = lax.shift_left(jnp.int32(1), lax.broadcasted_iota(jnp.int32, (32, block), 0))
    sum_row = lax.broadcasted_iota(jnp.int32, (tall - cols, block), 0)

    def entries(group):
        line = lax.shift_right_logical(group * GROUP, 7)
        start = (group * GROUP) & 127
        found = []
        for u in range(GROUP):
            value = list_ref[line, start + u]
            slot = value & ((1 << slot_bits) - 1)
            rest = lax.shift_right_logical(value, slot_bits)
            src = rest & ((1 << src_bits) - 1)
            rest = lax.shift_right_logical(rest, src_bits)
            rel = rest & ((1 << rel_bits) - 1)
            rest = lax.shift_right_logical(rest, rel_bits)
            dst = rest & ((1 << own_bits) - 1)
            valid = -lax.shift_right_logical(rest, own_bits)
            found.append((slot, src, rel, dst, valid))
        return found

    def turn(group):
        picks = entries(group)
        dst = picks[0][3]
        stack = jnp.concatenate([att_ref[rel] for _, _, rel, _, _ in picks], axis=0)
        turned = jnp.dot(stack, qt_ref[dst], preferred_element_type=jnp.float32)
        for u, (_, _, rel, _, _) in enumerate(picks):
            for k in range(heads):
                lo = u * cols + k * size
                scaled = turned[lo : lo + size] * (prior_ref[k, rel] * factor)
                right[u, k * size : (k + 1) * size, k * block : (k + 1) * block] = scaled.astype(jnp.bfloat16)

    def send_messages(group):
        for u, (_, src, rel, _, _) in enumerate(entries(group)):
            message = jnp.dot(msg_ref[rel], vt_ref[src], preferred_element_type=jnp.float32).astype(jnp.bfloat16)
            for k in range(heads):
                lo = u * span + k * block
                left[k * size : (k + 1) * size, lo : lo + block] = message[k * size : (k + 1) * size]

    def score(group):
        best = [None] * heads
        for u, (slot, src, _, _, valid) in enumerate(entries(group)):
            found = jnp.dot(k_ref[src], right[u], preferred_element_type=jnp.float32)
            tile_words = bits_ref[slot] & valid
            edges = jnp.concatenate([(tile_words[w : w + 1] & bit_of) != 0 for w in range(words)], axis=0)
            for k in range(heads):
                masked = jnp.where(edges, found[:, k * block : (k + 1) * block], NEG)
                scores[u * heads + k] = masked
                top = jnp.max(masked.reshape(block // 8, 8, block), axis=0)
                best[k] = top if best[k] is None else jnp.maximum(best[k], top)
        for k in range(heads):
            peak[k : k + 1] = jnp.max(best[k], axis=0, keepdims=True)

    def gather(group):
        dst = entries(group)[0][3]
        keeps, weights = [], [None] * (GROUP * heads)
        for k in range(heads):
            old = top_ref[dst, k : k + 1]
            new = jnp.maximum(old, peak[k : k + 1])
            top_ref[dst, k : k + 1] = new
            keeps.append(jnp.exp(old - new))
            for u in range(GROUP):
                weights[u * heads + k] = jnp.exp(scores[u * heads + k] - new).astype(jnp.bfloat16)
        out = jnp.dot(left[...], jnp.concatenate(weights, axis=0), preferred_element_type=jnp.float32)
        for k in range(heads):
            rows = slice(k * size, (k + 1) * size)
            acc_ref[dst, rows] = acc_ref[dst, rows] * keeps[k] + out[rows]
        keep = jnp.broadcast_to(keeps[0], sum_row.shape)
        for k in range(1, heads):
            keep = jnp.where(sum_row == k, keeps[k], keep)
        acc_ref[dst, cols:] = acc_ref[dst, cols:] * keep + out[cols:]

    def visit(group, carry):
        gather(group)
        score(group + 1)
        send_messages(group + 1)
        turn(group + 2)
        return carry

    turn(0)
    score(0)
    send_messages(0)
    turn(1)
    lax.fori_loop(0, groups, visit, 0)


def finish_kernel(n_rel, n_head, heads, acc_ref, types_ref, skip_ref, feat_ref, w_ref, *refs):
    out_ref, hid_out, hid_got, resid, send_sem, recv_sem, local = refs
    own_blocks, _, block = acc_ref.shape
    kinds = w_ref.shape[1]
    cols = w_ref.shape[2]
    width = w_ref.shape[3]
    size = cols // heads
    per = own_blocks // n_head
    piece = per * block
    r = lax.axis_index("rel")
    h = lax.axis_index("head")
    span = n_rel * piece

    fetch = pltpu.make_async_copy(feat_ref.at[pl.ds(pl.multiple_of(h * span, span), span)], resid, local.at[0])
    fetch.start()
    barrier = pltpu.get_barrier_semaphore()
    shifts = [(a, b) for b in range(n_head) for a in range(n_rel) if a or b]
    for a, b in shifts:
        target = {"rel": lax.rem(r + a, n_rel), "head": lax.rem(h + b, n_head)}
        pl.semaphore_signal(barrier, inc=1, device_id=target)

    def hidden_of(source):
        total = jnp.maximum(acc_ref[source, cols : cols + 8], 1.0)
        sides = []
        for k in range(heads):
            sides.append(acc_ref[source, pl.ds(k * size, size)] / total[k : k + 1])
        agg = jnp.concatenate(sides, axis=0)
        inner = math.sqrt(2.0 / math.pi) * (agg + 0.044715 * (agg * agg * agg))
        hidden = agg * (0.5 * (1.0 + jnp.tanh(inner)))
        return hidden.T.astype(jnp.bfloat16)

    for b in range(n_head):
        head = lax.rem(h + b, n_head)
        for i in range(per):
            hid_out[b, i * block : (i + 1) * block] = hidden_of(head * per + i)
    pl.semaphore_wait(barrier, len(shifts))

    sends = {}
    for a, b in sorted(shifts, key=lambda s: (s[0] == 0, s[1])):
        target = {"rel": lax.rem(r + a, n_rel), "head": lax.rem(h + b, n_head)}
        copy = pltpu.make_async_remote_copy(
            src_ref=hid_out.at[b],
            dst_ref=hid_got.at[a, b],
            send_sem=send_sem.at[a, b],
            recv_sem=recv_sem.at[a, b],
            device_id=target,
        )
        copy.start()
        sends[a, b] = copy
    hid_got[0, 0] = hid_out[0]
    fetch.wait()
    gates = []
    for a in range(n_rel):
        source = lax.rem(r + n_rel - a, n_rel)
        for b in range(n_head):
            if a or b:
                sends[a, b].wait_recv()
        parts = [hid_got[a, lax.rem(h + n_head - head, n_head)] for head in range(n_head)]
        hidden = jnp.concatenate(parts, axis=1)
        outs = []
        for kind in range(kinds):
            weights = jnp.concatenate([w_ref[head, kind] for head in range(n_head)], axis=0)
            outs.append(jnp.dot(hidden, weights, preferred_element_type=jnp.float32))
        for i in range(per):
            mask = column(types_ref[pl.ds((h * n_rel + source) * per + i, 1), :])
            masks = [mask == float(kind) for kind in range(kinds)]
            logit = jnp.full((block, block), skip_ref[0], jnp.float32)
            for kind in range(1, kinds):
                logit = jnp.where(masks[kind], skip_ref[kind], logit)
            gate = 1.0 / (1.0 + jnp.exp(-logit))
            rows = pl.ds(pl.multiple_of(source * piece + i * block, block), block)
            for w in range(width // block):
                lanes = slice(w * block, (w + 1) * block)
                total = outs[0][i * block : (i + 1) * block, lanes]
                for kind in range(1, kinds):
                    total = jnp.where(masks[kind], outs[kind][i * block : (i + 1) * block, lanes], total)
                old = resid[rows, lanes].astype(jnp.float32)
                out_ref[rows, lanes] = (gate * total + (1.0 - gate) * old).astype(jnp.bfloat16)
    for copy in sends.values():
        copy.wait_send()


def per_device(
    features,
    node_type,
    w_query,
    w_key,
    w_value,
    rel_att,
    rel_msg,
    rel_prior,
    w_out,
    skip,
    rel_perm,
    tile_src,
    tile_dst,
    tile_bits,
    tile_count,
):
    node_rows, width = features.shape
    n_rel = lax.axis_size("rel")
    n_node = lax.axis_size("node")
    n_head = lax.axis_size("head")
    relations, heads = rel_prior.shape
    cols = w_query.shape[2]
    kinds = w_query.shape[0]
    block = tile_bits.shape[2]
    words = tile_bits.shape[3]
    blocks = node_rows // block
    positions, tcap = tile_src.shape
    slots = positions * tcap
    factor = 1.0 / math.sqrt(cols // heads)
    own_blocks = blocks // n_rel
    all_slots = n_rel * slots
    bf = jnp.bfloat16
    fields = (
        bits_for(n_node * blocks),
        bits_for(blocks),
        bits_for(all_slots),
        bits_for(relations),
        bits_for(own_blocks),
    )

    bits = tile_bits.transpose(0, 1, 3, 2).reshape(slots, words, block)

    list_rows = -(-(all_slots + own_blocks * GROUP + 3 * GROUP) // block) + 1
    chunks = blocks // CHUNK
    half = max(n_head // 2 - 1, 1)
    dma = pltpu.SemaphoreType.DMA
    smem = pl.BlockSpec(memory_space=pltpu.SMEM)
    vmem = pl.BlockSpec(memory_space=pltpu.VMEM)
    hbm = pl.BlockSpec(memory_space=pltpu.HBM)
    shape = jax.ShapeDtypeStruct
    operands = (
        node_type.reshape(blocks, block),
        tile_src,
        tile_dst,
        tile_count.reshape(1, positions),
        rel_perm.reshape(1, positions),
        features,
        w_key,
        w_value,
        w_query,
        rel_att,
        rel_msg,
        w_out,
        bits,
    )
    keys, values_t, query_t, att, msg, all_bits, all_out, listed = pl.pallas_call(
        functools.partial(prepare_kernel, n_rel, n_node, n_head, fields),
        in_specs=[hbm] * 13,
        out_specs=[vmem] * 8,
        out_shape=[
            shape((n_node * blocks, block, cols), bf),
            shape((n_node * blocks, cols, block), bf),
            shape((own_blocks, cols, block), bf),
            shape((relations, cols, cols), bf),
            shape((relations, cols, cols), bf),
            shape((all_slots, words, block), jnp.int32),
            shape((n_head,) + w_out.shape, bf),
            shape((list_rows, block), jnp.int32),
        ],
        scratch_shapes=[
            pltpu.VMEM(features.shape, bf),
            pltpu.VMEM(w_key.shape, bf),
            pltpu.VMEM(w_value.shape, bf),
            pltpu.VMEM(w_query.shape, bf),
            pltpu.VMEM(rel_att.shape, bf),
            pltpu.VMEM(rel_msg.shape, bf),
            pltpu.VMEM((n_rel, 8, block), jnp.int32),
            pltpu.VMEM((blocks, block), jnp.int32),
            pltpu.VMEM((positions, tcap), jnp.int32),
            pltpu.VMEM((positions, tcap), jnp.int32),
            pltpu.VMEM((1, positions), jnp.int32),
            pltpu.VMEM((1, positions), jnp.int32),
            dma((13 + chunks,)),
            dma((n_rel,)),
            dma((n_rel,)),
            dma((n_rel, half)),
            dma((n_rel, half)),
            dma((n_rel, 1 + half)),
            dma((n_rel, 1 + half)),
            dma((n_rel,)),
            dma((n_rel,)),
            dma((n_node, chunks, 2)),
            dma((n_node, chunks, 2)),
            dma((n_head,)),
            dma((n_head,)),
        ],
        compiler_params=pltpu.CompilerParams(collective_id=0, has_side_effects=True, vmem_limit_bytes=VMEM_BYTES),
        name="prepare",
    )(*[in_hbm(value) for value in operands])

    tall = cols + PAD_ROWS
    acc = pl.pallas_call(
        functools.partial(tile_kernel, heads, factor, fields),
        in_specs=[smem] * 2 + [vmem] * 6,
        out_specs=vmem,
        out_shape=shape((own_blocks, tall, block), jnp.float32),
        scratch_shapes=[
            pltpu.VMEM((own_blocks, 8, block), jnp.float32),
            pltpu.VMEM((tall, GROUP * heads * block), bf),
            pltpu.VMEM((GROUP, cols, heads * block), bf),
            pltpu.VMEM((GROUP * heads, block, block), jnp.float32),
            pltpu.VMEM((8, block), jnp.float32),
        ],
        compiler_params=pltpu.CompilerParams(vmem_limit_bytes=VMEM_BYTES),
        name="tiles",
    )(listed, rel_prior.T, query_t, keys, values_t, all_bits, att, msg)

    piece = own_blocks // n_head * block
    return pl.pallas_call(
        functools.partial(finish_kernel, n_rel, n_head, heads),
        in_specs=[vmem, vmem, smem, hbm, vmem],
        out_specs=vmem,
        out_shape=shape((n_rel * piece, width), bf),
        scratch_shapes=[
            pltpu.VMEM((n_head, piece, cols), bf),
            pltpu.VMEM((n_rel, n_head, piece, cols), bf),
            pltpu.VMEM((n_rel * piece, width), bf),
            dma((n_rel, n_head)),
            dma((n_rel, n_head)),
            dma((1,)),
        ],
        compiler_params=pltpu.CompilerParams(collective_id=1, has_side_effects=True, vmem_limit_bytes=VMEM_BYTES),
        name="finish",
    )(acc, node_type.reshape(blocks, block), skip, in_hbm(features), all_out)


def solution(mesh):
    in_specs = (
        P("node", None),
        P("node"),
        P(None, None, "head"),
        P(None, None, "head"),
        P(None, None, "head"),
        P(None, "head", None, None),
        P(None, "head", None, None),
        P(None, "head"),
        P(None, "head", None),
        P(),
        P("rel"),
        P("rel", "node"),
        P("rel", "node"),
        P("rel", "node", None, None),
        P("rel", "node"),
    )
    out_specs = P(("node", "head"), None)
    return jax.shard_map(
        per_device, mesh=mesh, in_specs=in_specs, out_specs=out_specs, check_vma=False
    )
```

```python
import functools
import math

import jax
import jax.numpy as jnp
from jax import lax
from jax.experimental import pallas as pl
from jax.experimental.pallas import tpu as pltpu
from jax.sharding import PartitionSpec as P

NEG = -1e30
FLOOR = -1e29
GROUP = 4
CHUNK = 4
SPLIT = 3
BATCH = 8
PAD_ROWS = 16
VMEM_BYTES = 30 * 1024 * 1024


def column(types_row):
    size = types_row.shape[1]
    return jnp.broadcast_to(types_row.astype(jnp.float32), (size, size)).T


def in_hbm(value):
    return pltpu.with_memory_space_constraint(value, pltpu.HBM)


def bits_for(count):
    return max(int(count - 1).bit_length(), 1)


def own_block(local, per, n_rel, r):
    return (local // per) * per * n_rel + r * per + local % per


def project_rows(x, weights):
    return [jnp.dot(x, w, preferred_element_type=jnp.float32) for w in weights]


def compact(meta, own_blocks, per, n_rel, r, fields, list_ref):
    src_bits, dst_bits, slot_bits, rel_bits, own_bits = fields
    rows, lanes = meta.shape
    live = meta >= 0
    src = meta & ((1 << src_bits) - 1)
    dst = lax.shift_right_logical(meta, src_bits) & ((1 << dst_bits) - 1)
    rel = lax.shift_right_logical(meta, src_bits + dst_bits) & ((1 << rel_bits) - 1)
    slot = lax.broadcasted_iota(jnp.int32, meta.shape, 0) * lanes + lax.broadcasted_iota(jnp.int32, meta.shape, 1)
    base = slot | lax.shift_left(src, slot_bits) | lax.shift_left(rel, slot_bits + src_bits)
    top = slot_bits + src_bits + rel_bits
    base = base | (1 << (top + own_bits))
    bf = jnp.bfloat16
    hits = [live & (dst == own_block(d, per, n_rel, r)) for d in range(own_blocks)]
    flags = jnp.concatenate([jnp.where(hit, 1.0, 0.0) for hit in hits], axis=0).astype(bf)
    size = own_blocks * rows
    before = lax.broadcasted_iota(jnp.int32, (lanes, lanes), 0) < lax.broadcasted_iota(jnp.int32, (lanes, lanes), 1)
    in_row = jnp.dot(flags, jnp.where(before, 1.0, 0.0).astype(bf), preferred_element_type=jnp.float32)
    row_sum = jnp.dot(flags, jnp.ones((lanes, lanes), bf), preferred_element_type=jnp.float32).astype(bf)
    i = lax.broadcasted_iota(jnp.int32, (size, size), 0)
    j = lax.broadcasted_iota(jnp.int32, (size, size), 1)
    same = jnp.zeros((size, size), jnp.bool_)
    for d in range(own_blocks):
        lo, hi = d * rows, (d + 1) * rows
        same = same | ((i >= lo) & (i < hi) & (j >= lo) & (j < hi))
    ahead = jnp.where(same & (j < i), 1.0, 0.0).astype(bf)
    both = jnp.where(same, 1.0, 0.0).astype(bf)
    rows_before = jnp.dot(ahead, row_sum, preferred_element_type=jnp.float32)
    totals = jnp.dot(both, row_sum, preferred_element_type=jnp.float32)
    rank = jnp.full(meta.shape, -1.0, jnp.float32)
    entry = base
    start = jnp.zeros(meta.shape, jnp.float32)
    for d in range(own_blocks):
        part = slice(d * rows, (d + 1) * rows)
        place = start + rows_before[part] + in_row[part]
        rank = jnp.where(hits[d], place, rank)
        entry = jnp.where(hits[d], base | (d << top), entry)
        start = start + jnp.floor((totals[part] + (GROUP - 1)) * (1.0 / GROUP)) * GROUP
    pieces = [(lax.shift_right_logical(entry, 8 * q) & 255).astype(jnp.float32) for q in range(4)]
    row_entries = []
    for a in range(rows):
        parts = [piece[a : a + 1] for piece in pieces] + [jnp.zeros((4, lanes), jnp.float32)]
        row_entries.append(jnp.concatenate(parts, axis=0).astype(bf))
    places = lax.broadcasted_iota(jnp.int32, (lanes, lanes), 0).astype(jnp.float32)
    for k in range(list_ref.shape[0] - 1):
        ids = places + float(k * lanes)
        found = jnp.zeros((8, lanes), jnp.float32)
        for a in range(rows):
            hot = jnp.where(ids == rank[a : a + 1], 1.0, 0.0).astype(bf)
            found = found + lax.dot_general(
                row_entries[a], hot, (((1,), (1,)), ((), ())), preferred_element_type=jnp.float32
            )
        whole = found.astype(jnp.int32)
        line = whole[0:1]
        for q in range(1, 4):
            line = line | lax.shift_left(whole[q : q + 1], 8 * q)
        list_ref[k : k + 1] = line
    groups = (start[0:1] * (1.0 / GROUP)).astype(jnp.int32)
    list_ref[list_ref.shape[0] - 1 :] = groups


def pack(src, dst, count, perm, fields, lanes):
    positions, tcap = src.shape
    i = lax.broadcasted_iota(jnp.int32, (positions, positions), 0)
    j = lax.broadcasted_iota(jnp.int32, (positions, positions), 1)

    def upright(row):
        return jnp.sum(jnp.where(i == j, row.astype(jnp.float32), 0.0), axis=1, keepdims=True).astype(jnp.int32)

    word = src | lax.shift_left(dst, fields[0]) | lax.shift_left(upright(perm), fields[0] + fields[1])
    slot = lax.broadcasted_iota(jnp.int32, src.shape, 1)
    word = jnp.where(slot < upright(count), word, -1)
    each = lanes // tcap
    rows = [
        jnp.concatenate([word[a + b : a + b + 1] for b in range(each)], axis=1) for a in range(0, positions, each)
    ]
    rows.append(jnp.full((8 - len(rows), lanes), -1, jnp.int32))
    return jnp.concatenate(rows, axis=0).reshape(1, 8, lanes)


def prepare_kernel(n_rel, n_node, n_head, fields, *refs):
    (small, feat_ref, wk_ref, wv_ref, wq_ref, msg_ref, bits_ref), refs = (
        (refs[:5],) + refs[5:11],
        refs[11:],
    )
    (kv_all, qt_ref, msg_out, bits_all, list_ref) = refs[:5]
    (x_v, wk_v, wv_v, wq_v, msg_v, meta_all), refs = refs[5:11], refs[11:]
    (types_ref, src_v, dst_v, count_v, perm_v), refs = refs[:5], refs[5:]
    (local, z_send, z_recv, y_send, y_recv, d_send, d_recv, m_send, m_recv, x_send, x_recv, f_send, f_recv) = refs
    blocks = types_ref.shape[0]
    block = types_ref.shape[1]
    cols = wk_v.shape[2]
    kinds = wk_v.shape[0]
    slots = bits_ref.shape[0]
    share = slots // n_head
    own_blocks = qt_ref.shape[0]
    per = own_blocks // n_head
    chunks = blocks // CHUNK
    rows = CHUNK * block
    relations, heads, size = msg_v.shape[:3]
    r = lax.axis_index("rel")
    n = lax.axis_index("node")
    h = lax.axis_index("head")
    sibling = h + 1 - 2 * lax.rem(h, 2)
    parity = lax.rem(r, 2)
    partner = r + 1 - 2 * parity
    pairs = list(range(2, n_head, 2))
    bf = jnp.bfloat16

    def fetch(src, dst, index):
        copy = pltpu.make_async_copy(src, dst, local.at[index])
        copy.start()
        return copy

    small_v = (types_ref, src_v, dst_v, count_v, perm_v)
    got_small = [fetch(a, b, 8 + chunks + i) for i, (a, b) in enumerate(zip(small, small_v))]
    own_bits = fetch(bits_ref, bits_all.at[pl.ds(pl.multiple_of(r * slots, slots), slots)], 0)
    got_w = [fetch(wk_ref, wk_v, 1), fetch(wv_ref, wv_v, 2)]
    got_x = []
    for c in range(chunks):
        got_x.append(fetch(feat_ref.at[pl.ds(c * rows, rows)], x_v.at[pl.ds(c * rows, rows)], 8 + c))
    got_q = fetch(wq_ref, wq_v, 3)
    got_rel = fetch(msg_ref, msg_v, 4)

    barrier = pltpu.get_barrier_semaphore()
    for t in range(1, n_rel):
        pl.semaphore_signal(barrier, inc=1, device_id={"rel": lax.rem(r + t, n_rel)})
    for t in range(1, n_node):
        pl.semaphore_signal(barrier, inc=1, device_id={"node": lax.rem(n + t, n_node)})
    for t in pairs:
        pl.semaphore_signal(barrier, inc=1, device_id={"head": lax.rem(h + t, n_head)})
    pl.semaphore_signal(barrier, inc=1, device_id={"head": sibling})
    for copy in got_small:
        copy.wait()
    meta_all[pl.ds(r, 1)] = pack(src_v[...], dst_v[...], count_v[...], perm_v[...], fields, block)
    pl.semaphore_wait(barrier, n_rel - 1 + n_node - 1 + len(pairs) + 1)

    started = []

    def send(src, dst, send_sem, recv_sem, target):
        copy = pltpu.make_async_remote_copy(
            src_ref=src, dst_ref=dst, send_sem=send_sem, recv_sem=recv_sem, device_id=target
        )
        copy.start()
        started.append(copy)
        return copy

    def bit_rows(rel, head):
        return bits_all.at[pl.ds(pl.multiple_of(rel * slots + head * share, share), share)]

    own_bits.wait()
    metas, zs = [], []
    for t in range(1, n_rel):
        target = {"rel": lax.rem(r + t, n_rel)}
        metas.append(send(meta_all.at[r], meta_all.at[r], m_send.at[t], m_recv.at[t], target))
    for t in range(1, n_rel):
        target = {"rel": lax.rem(r + t, n_rel)}
        zs.append(send(bit_rows(r, h), bit_rows(r, h), z_send.at[t], z_recv.at[t], target))

    for copy in got_w:
        copy.wait()
    xs, halves = [], []
    for c in range(chunks):
        got_x[c].wait()
        x = x_v[c * rows : (c + 1) * rows]
        masks = [column(types_ref[c * CHUNK + b : c * CHUNK + b + 1, :]) for b in range(CHUNK)]
        totals = [None] * CHUNK
        for kind in range(kinds):
            both = jnp.concatenate([wk_v[kind], wv_v[kind]], axis=1)
            out = jnp.dot(x, both, preferred_element_type=jnp.float32)
            for b in range(CHUNK):
                piece = out[b * block : (b + 1) * block]
                pair = (piece[:, :cols], piece[:, cols:])
                if totals[b] is None:
                    totals[b] = pair
                else:
                    hit = masks[b] == float(kind)
                    totals[b] = tuple(jnp.where(hit, new, old) for new, old in zip(pair, totals[b]))
        first = n * blocks + c * CHUNK
        for b in range(CHUNK):
            kv_all[0, first + b] = totals[b][0].astype(bf)
            kv_all[1, first + b] = totals[b][1].T.astype(bf)
        for t in range(1, n_node):
            target = {"node": lax.rem(n + t, n_node)}
            if c < SPLIT:
                part = kv_all.at[parity, pl.ds(first, CHUNK)]
                halves.append((t, c, send(part, part, x_send.at[t, c, 0], x_recv.at[t, c, 0], target)))
            else:
                for which in range(2):
                    part = kv_all.at[which, pl.ds(first, CHUNK)]
                    xs.append(send(part, part, x_send.at[t, c, which], x_recv.at[t, c, which], target))

    def forward(chunk):
        for t, c, copy in halves:
            if c == chunk:
                copy.wait_recv()
                first = lax.rem(n + n_node - t, n_node) * blocks + c * CHUNK
                part = kv_all.at[parity, pl.ds(first, CHUNK)]
                xs.append(send(part, part, f_send.at[t, c], f_recv.at[t, c], {"rel": partner}))

    got_q.wait()
    wide = jnp.concatenate([wq_v[kind] for kind in range(kinds)], axis=1)
    mine = [own_block(d, per, n_rel, r) for d in range(own_blocks)]
    x = jnp.concatenate([x_v[pl.ds(pl.multiple_of(b * block, block), block)] for b in mine], axis=0)
    out = jnp.dot(x, wide, preferred_element_type=jnp.float32)
    for d in range(own_blocks):
        mask = column(types_ref[pl.ds(mine[d], 1), :])
        piece = out[d * block : (d + 1) * block]
        total = piece[:, :cols]
        for kind in range(1, kinds):
            total = jnp.where(mask == float(kind), piece[:, kind * cols : (kind + 1) * cols], total)
        qt_ref[d] = total.T.astype(bf)

    got_rel.wait()
    unit = lax.broadcasted_iota(jnp.int32, (size, size), 0) == lax.broadcasted_iota(jnp.int32, (size, size), 1)
    unit = jnp.where(unit, 1.0, 0.0).astype(bf)
    owner = lax.broadcasted_iota(jnp.int32, (size, cols), 1) // size

    def relation(index, carry):
        flat = msg_v[pl.ds(index * BATCH, BATCH)].reshape(BATCH * cols, size)
        turned = lax.dot_general(unit, flat, (((1,), (1,)), ((), ())), preferred_element_type=jnp.float32)
        for i in range(BATCH):
            both = turned[:, i * cols : (i + 1) * cols]
            for k in range(heads):
                part = jnp.where(owner == k, both, 0.0).astype(bf)
                msg_out[index * BATCH + i, k * size : (k + 1) * size] = part
        return carry

    ys, ds = [], []
    for t in range(1, n_rel):
        zs[t - 1].wait_recv()
        source = lax.rem(r + n_rel - t, n_rel)
        for i, u in enumerate(pairs):
            target = {"head": lax.rem(h + u, n_head)}
            ys.append((t, u, send(bit_rows(source, h), bit_rows(source, h), y_send.at[t, i], y_recv.at[t, i], target)))
        ds.append(
            send(bit_rows(source, h), bit_rows(source, h), d_send.at[t, 0], d_recv.at[t, 0], {"head": sibling})
        )
        if t == 1:
            lax.fori_loop(0, relations // BATCH, relation, 0)
            for copy in metas:
                copy.wait_recv()
            used = slots // block
            meta = jnp.concatenate([meta_all[s, :used] for s in range(n_rel)], axis=0)
            compact(meta, own_blocks, per, n_rel, r, fields, list_ref)
        if t - 1 < SPLIT:
            forward(t - 1)

    for c in range(n_rel - 1, SPLIT):
        forward(c)
    for t, u, copy in ys:
        copy.wait_recv()
        source = lax.rem(r + n_rel - t, n_rel)
        head = lax.rem(h + n_head - u, n_head)
        which = 1 + pairs.index(u)
        ds.append(
            send(bit_rows(source, head), bit_rows(source, head), d_send.at[t, which], d_recv.at[t, which], {"head": sibling})
        )
    for copy in ds:
        copy.wait_recv()
    for copy in xs:
        copy.wait_recv()
    for copy in started:
        copy.wait_send()


def tile_kernel(heads, factor, fields, list_ref, prior_ref, qt_ref, kv_ref, bits_ref, att_ref, msg_ref, *refs):
    acc_ref, top_ref = refs[:2]
    lefts, rights, scoress, peaks = refs[2:4], refs[4:6], refs[6:8], refs[8:10]
    src_bits, _, slot_bits, rel_bits, own_bits = fields
    own_blocks, cols, block = qt_ref.shape
    size = cols // heads
    words = bits_ref.shape[1]
    tall = acc_ref.shape[2]
    groups = list_ref[list_ref.shape[0] - 1, 0]

    acc_ref[...] = jnp.zeros_like(acc_ref)
    top_ref[...] = jnp.full_like(top_ref, FLOOR)
    for right in rights:
        right[...] = jnp.zeros_like(right)
    row = lax.broadcasted_iota(jnp.int32, (tall - size, GROUP * block), 0)
    ones = jnp.where(row == 0, 1.0, 0.0).astype(jnp.bfloat16)
    for left in lefts:
        for k in range(heads):
            left[k, size:] = ones
    bit_of = lax.shift_left(jnp.int32(1), lax.broadcasted_iota(jnp.int32, (32, block), 0))

    def entries(group):
        line = lax.shift_right_logical(group * GROUP, 7)
        start = (group * GROUP) & 127
        found = []
        for u in range(GROUP):
            value = list_ref[line, start + u]
            slot = value & ((1 << slot_bits) - 1)
            rest = lax.shift_right_logical(value, slot_bits)
            src = rest & ((1 << src_bits) - 1)
            rest = lax.shift_right_logical(rest, src_bits)
            rel = rest & ((1 << rel_bits) - 1)
            rest = lax.shift_right_logical(rest, rel_bits)
            dst = rest & ((1 << own_bits) - 1)
            valid = -lax.shift_right_logical(rest, own_bits)
            found.append((slot, src, rel, dst, valid))
        return found

    def turned_of(picks):
        dst = picks[0][3]
        found = []
        for k in range(heads):
            stack = jnp.concatenate([att_ref[rel, k] for _, _, rel, _, _ in picks], axis=0)
            query = qt_ref[dst, k * size : (k + 1) * size]
            found.append(jnp.dot(stack, query, preferred_element_type=jnp.float32))
        return found

    def keep_turned(picks, turned, right):
        for u, (_, _, rel, _, _) in enumerate(picks):
            for k in range(heads):
                scaled = turned[k][u * size : (u + 1) * size] * (prior_ref[k, rel] * factor)
                right[u, k * size : (k + 1) * size, k * block : (k + 1) * block] = scaled.astype(jnp.bfloat16)

    def messages_of(picks):
        return [jnp.dot(msg_ref[rel], kv_ref[1, src], preferred_element_type=jnp.float32) for _, src, rel, _, _ in picks]

    def keep_messages(messages, left):
        for u, message in enumerate(messages):
            for k in range(heads):
                lo = u * block
                left[k, :size, lo : lo + block] = message[k * size : (k + 1) * size].astype(jnp.bfloat16)

    def scores_of(picks, right):
        return [
            jnp.dot(kv_ref[0, src], right[u], preferred_element_type=jnp.float32)
            for u, (_, src, _, _, _) in enumerate(picks)
        ]

    def keep_scores(picks, found, scores, peak):
        best = [None] * heads
        for u, (slot, _, _, _, valid) in enumerate(picks):
            tile_words = bits_ref[slot] & valid
            edges = jnp.concatenate([(tile_words[w : w + 1] & bit_of) != 0 for w in range(words)], axis=0)
            for k in range(heads):
                masked = jnp.where(edges, found[u][:, k * block : (k + 1) * block], NEG)
                scores[u * heads + k] = masked
                top = jnp.max(masked.reshape(block // 8, 8, block), axis=0)
                best[k] = top if best[k] is None else jnp.maximum(best[k], top)
        for k in range(heads):
            peak[k : k + 1] = jnp.max(best[k], axis=0, keepdims=True)

    def gather(dst, left, scores, peak):
        outs = []
        for k in range(heads):
            old = top_ref[dst, k : k + 1]
            new = jnp.maximum(old, peak[k : k + 1])
            top_ref[dst, k : k + 1] = new
            weights = [jnp.exp(scores[u * heads + k] - new).astype(jnp.bfloat16) for u in range(GROUP)]
            out = jnp.dot(left[k], jnp.concatenate(weights, axis=0), preferred_element_type=jnp.float32)
            outs.append((jnp.exp(old - new), out))
        for k, (keep, out) in enumerate(outs):
            acc_ref[dst, k] = acc_ref[dst, k] * keep + out

    def visit(pair, carry):
        picks = [entries(pair * 2 + i) for i in range(4)]
        for i in range(2):
            now, soon, later = picks[i : i + 3]
            this, other = i, 1 - i
            keep_messages(messages_of(soon), lefts[other])
            found = scores_of(soon, rights[other])
            keep_turned(later, turned_of(later), rights[this])
            gather(now[0][3], lefts[this], scoress[this], peaks[this])
            keep_scores(soon, found, scoress[other], peaks[other])
        return carry

    first = entries(0)
    keep_turned(first, turned_of(first), rights[0])
    keep_scores(first, scores_of(first, rights[0]), scoress[0], peaks[0])
    keep_messages(messages_of(first), lefts[0])
    first = entries(1)
    keep_turned(first, turned_of(first), rights[1])
    lax.fori_loop(0, lax.shift_right_logical(groups + 1, 1), visit, 0)


def finish_kernel(n_rel, n_head, heads, acc_ref, types_ref, skip_ref, feat_ref, *refs):
    outs_w, refs = refs[: n_head // 2], refs[n_head // 2 :]
    out_ref, hid_out, hid_got, resid, w_ref, send_sem, recv_sem, w_send, w_recv, local = refs
    own_blocks, _, _, block = acc_ref.shape
    kinds = w_ref.shape[1]
    cols = w_ref.shape[2]
    width = w_ref.shape[3]
    size = cols // heads
    per = own_blocks // n_head
    piece = per * block
    r = lax.axis_index("rel")
    h = lax.axis_index("head")
    span = n_rel * piece

    fetch = pltpu.make_async_copy(feat_ref.at[pl.ds(pl.multiple_of(h * span, span), span)], resid, local.at[0])
    fetch.start()
    loads = []
    for i, got in enumerate(outs_w):
        head = lax.rem(h + n_head - 2 * i, n_head)
        loads.append((head, pltpu.make_async_copy(got, w_ref.at[head], local.at[1 + i])))
        loads[-1][1].start()
    barrier = pltpu.get_barrier_semaphore()
    shifts = [(a, b) for b in range(n_head) for a in range(n_rel) if a or b]
    for a, b in shifts:
        target = {"rel": lax.rem(r + a, n_rel), "head": lax.rem(h + b, n_head)}
        pl.semaphore_signal(barrier, inc=1, device_id=target)

    def hidden_of(source):
        sides = []
        for k in range(heads):
            total = jnp.maximum(acc_ref[source, k, size : size + 1], 1.0)
            sides.append(acc_ref[source, k, :size] / total)
        agg = jnp.concatenate(sides, axis=0)
        inner = math.sqrt(2.0 / math.pi) * (agg + 0.044715 * (agg * agg * agg))
        hidden = agg * (0.5 * (1.0 + jnp.tanh(inner)))
        return hidden.T.astype(jnp.bfloat16)

    for b in range(n_head):
        head = lax.rem(h + b, n_head)
        for i in range(per):
            hid_out[b, i * block : (i + 1) * block] = hidden_of(head * per + i)
    pl.semaphore_wait(barrier, len(shifts))

    sends = {}
    for a, b in sorted(shifts, key=lambda s: (s[0] == 0, s[1])):
        target = {"rel": lax.rem(r + a, n_rel), "head": lax.rem(h + b, n_head)}
        copy = pltpu.make_async_remote_copy(
            src_ref=hid_out.at[b],
            dst_ref=hid_got.at[a, b],
            send_sem=send_sem.at[a, b],
            recv_sem=recv_sem.at[a, b],
            device_id=target,
        )
        copy.start()
        sends[a, b] = copy
    hid_got[0, 0] = hid_out[0]
    shared = []
    for i, (head, load) in enumerate(loads):
        load.wait()
        copy = pltpu.make_async_remote_copy(
            src_ref=w_ref.at[head],
            dst_ref=w_ref.at[head],
            send_sem=w_send.at[i],
            recv_sem=w_recv.at[i],
            device_id={"head": h + 1 - 2 * lax.rem(h, 2)},
        )
        copy.start()
        shared.append(copy)
    fetch.wait()
    for copy in shared:
        copy.wait_recv()
    for a in range(n_rel):
        source = lax.rem(r + n_rel - a, n_rel)
        for b in range(n_head):
            if a or b:
                sends[a, b].wait_recv()
        parts = [hid_got[a, lax.rem(h + n_head - head, n_head)] for head in range(n_head)]
        hidden = jnp.concatenate(parts, axis=1)
        outs = []
        for kind in range(kinds):
            weights = jnp.concatenate([w_ref[head, kind] for head in range(n_head)], axis=0)
            outs.append(jnp.dot(hidden, weights, preferred_element_type=jnp.float32))
        for i in range(per):
            mask = column(types_ref[pl.ds((h * n_rel + source) * per + i, 1), :])
            masks = [mask == float(kind) for kind in range(kinds)]
            logit = jnp.full((block, block), skip_ref[0], jnp.float32)
            for kind in range(1, kinds):
                logit = jnp.where(masks[kind], skip_ref[kind], logit)
            gate = 1.0 / (1.0 + jnp.exp(-logit))
            rows = pl.ds(pl.multiple_of(source * piece + i * block, block), block)
            for w in range(width // block):
                lanes = slice(w * block, (w + 1) * block)
                total = outs[0][i * block : (i + 1) * block, lanes]
                for kind in range(1, kinds):
                    total = jnp.where(masks[kind], outs[kind][i * block : (i + 1) * block, lanes], total)
                old = resid[rows, lanes].astype(jnp.float32)
                out_ref[rows, lanes] = (gate * total + (1.0 - gate) * old).astype(jnp.bfloat16)
    for copy in list(sends.values()) + shared:
        copy.wait_send()


def per_device(
    features,
    node_type,
    w_query,
    w_key,
    w_value,
    rel_att,
    rel_msg,
    rel_prior,
    w_out,
    skip,
    rel_perm,
    tile_src,
    tile_dst,
    tile_bits,
    tile_count,
):
    node_rows, width = features.shape
    n_rel = lax.axis_size("rel")
    n_node = lax.axis_size("node")
    n_head = lax.axis_size("head")
    relations, heads = rel_prior.shape
    cols = w_query.shape[2]
    kinds = w_query.shape[0]
    block = tile_bits.shape[2]
    words = tile_bits.shape[3]
    blocks = node_rows // block
    positions, tcap = tile_src.shape
    slots = positions * tcap
    factor = 1.0 / math.sqrt(cols // heads)
    own_blocks = blocks // n_rel
    all_slots = n_rel * slots
    bf = jnp.bfloat16
    fields = (
        bits_for(n_node * blocks),
        bits_for(blocks),
        bits_for(all_slots),
        bits_for(relations),
        bits_for(own_blocks),
    )

    bits = tile_bits.transpose(0, 1, 3, 2).reshape(slots, words, block)

    list_rows = -(-(all_slots + own_blocks * GROUP + 4 * GROUP) // block) + 1
    chunks = blocks // CHUNK
    half = max(n_head // 2 - 1, 1)
    dma = pltpu.SemaphoreType.DMA
    smem = pl.BlockSpec(memory_space=pltpu.SMEM)
    vmem = pl.BlockSpec(memory_space=pltpu.VMEM)
    hbm = pl.BlockSpec(memory_space=pltpu.HBM)
    shape = jax.ShapeDtypeStruct
    operands = (
        node_type.reshape(blocks, block),
        tile_src,
        tile_dst,
        tile_count.reshape(1, positions),
        rel_perm.reshape(1, positions),
        features,
        w_key,
        w_value,
        w_query,
        rel_msg,
        bits,
    )
    pairs_kv, query_t, msg, all_bits, listed = pl.pallas_call(
        functools.partial(prepare_kernel, n_rel, n_node, n_head, fields),
        in_specs=[hbm] * 11,
        out_specs=[vmem] * 5,
        out_shape=[
            shape((2, n_node * blocks, block, cols), bf),
            shape((own_blocks, cols, block), bf),
            shape((relations, cols, cols), bf),
            shape((all_slots, words, block), jnp.int32),
            shape((list_rows, block), jnp.int32),
        ],
        scratch_shapes=[
            pltpu.VMEM(features.shape, bf),
            pltpu.VMEM(w_key.shape, bf),
            pltpu.VMEM(w_value.shape, bf),
            pltpu.VMEM(w_query.shape, bf),
            pltpu.VMEM(rel_msg.shape, bf),
            pltpu.VMEM((n_rel, 8, block), jnp.int32),
            pltpu.VMEM((blocks, block), jnp.int32),
            pltpu.VMEM((positions, tcap), jnp.int32),
            pltpu.VMEM((positions, tcap), jnp.int32),
            pltpu.VMEM((1, positions), jnp.int32),
            pltpu.VMEM((1, positions), jnp.int32),
            dma((13 + chunks,)),
            dma((n_rel,)),
            dma((n_rel,)),
            dma((n_rel, half)),
            dma((n_rel, half)),
            dma((n_rel, 1 + half)),
            dma((n_rel, 1 + half)),
            dma((n_rel,)),
            dma((n_rel,)),
            dma((n_node, chunks, 2)),
            dma((n_node, chunks, 2)),
            dma((n_node, chunks)),
            dma((n_node, chunks)),
        ],
        compiler_params=pltpu.CompilerParams(collective_id=0, has_side_effects=True, vmem_limit_bytes=VMEM_BYTES),
        name="prepare",
    )(*[in_hbm(value) for value in operands])

    tall = cols // heads + PAD_ROWS
    acc = pl.pallas_call(
        functools.partial(tile_kernel, heads, factor, fields),
        in_specs=[smem] * 2 + [vmem] * 5,
        out_specs=vmem,
        out_shape=shape((own_blocks, heads, tall, block), jnp.float32),
        scratch_shapes=[
            pltpu.VMEM((own_blocks, 8, block), jnp.float32),
            *[pltpu.VMEM((heads, tall, GROUP * block), bf)] * 2,
            *[pltpu.VMEM((GROUP, cols, heads * block), bf)] * 2,
            *[pltpu.VMEM((GROUP * heads, block, block), jnp.float32)] * 2,
            *[pltpu.VMEM((8, block), jnp.float32)] * 2,
        ],
        compiler_params=pltpu.CompilerParams(vmem_limit_bytes=VMEM_BYTES),
        name="tiles",
    )(listed, rel_prior.T, query_t, pairs_kv, all_bits, rel_att, msg)

    gathered = [w_out]
    for shift in range(2, n_head, 2):
        pairs = [(i, (i + shift) % n_head) for i in range(n_head)]
        gathered.append(lax.ppermute(w_out, "head", pairs))
    piece = own_blocks // n_head * block
    return pl.pallas_call(
        functools.partial(finish_kernel, n_rel, n_head, heads),
        in_specs=[vmem, vmem, smem, hbm, hbm] + [vmem] * (len(gathered) - 1),
        out_specs=vmem,
        out_shape=shape((n_rel * piece, width), bf),
        scratch_shapes=[
            pltpu.VMEM((n_head, piece, cols), bf),
            pltpu.VMEM((n_rel, n_head, piece, cols), bf),
            pltpu.VMEM((n_rel * piece, width), bf),
            pltpu.VMEM((n_head,) + w_out.shape, bf),
            dma((n_rel, n_head)),
            dma((n_rel, n_head)),
            dma((n_head,)),
            dma((n_head,)),
            dma((1 + n_head,)),
        ],
        compiler_params=pltpu.CompilerParams(collective_id=1, has_side_effects=True, vmem_limit_bytes=VMEM_BYTES),
        name="finish",
    )(acc, node_type.reshape(blocks, block), skip, in_hbm(features), in_hbm(w_out), *gathered[1:])


def solution(mesh):
    in_specs = (
        P("node", None),
        P("node"),
        P(None, None, "head"),
        P(None, None, "head"),
        P(None, None, "head"),
        P(None, "head", None, None),
        P(None, "head", None, None),
        P(None, "head"),
        P(None, "head", None),
        P(),
        P("rel"),
        P("rel", "node"),
        P("rel", "node"),
        P("rel", "node", None, None),
        P("rel", "node"),
    )
    out_specs = P(("node", "head"), None)
    return jax.shard_map(
        per_device, mesh=mesh, in_specs=in_specs, out_specs=out_specs, check_vma=False
    )
```

```python
import functools
import math

import jax
import jax.numpy as jnp
from jax import lax
from jax.experimental import pallas as pl
from jax.experimental.pallas import tpu as pltpu
from jax.sharding import PartitionSpec as P

NEG = -1e30
FLOOR = -1e29
GROUP = 4
CHUNK = 4
SPLIT = 3
BATCH = 8
PIECES = 2
PAD_ROWS = 16
VMEM_BYTES = 30 * 1024 * 1024


def column(types_row):
    size = types_row.shape[1]
    return jnp.broadcast_to(types_row.astype(jnp.float32), (size, size)).T


def in_hbm(value):
    return pltpu.with_memory_space_constraint(value, pltpu.HBM)


def bits_for(count):
    return max(int(count - 1).bit_length(), 1)


def own_block(local, per, n_rel, r):
    return (local // per) * per * n_rel + r * per + local % per


def along_rel(n_rel, r):
    if n_rel == 4:
        peers = {2: lax.rem(r + 2, 4), 1: r + 1 - 2 * lax.rem(r, 2), 3: 3 - r}
        return {u: (peer, peer) for u, peer in peers.items()}, (r == 1) | (r == 2)
    return {u: (lax.rem(r + u, n_rel), lax.rem(r + n_rel - u, n_rel)) for u in range(1, n_rel)}, None


def only_if(condition, action):
    if condition is None:
        action()
    else:
        pl.when(condition)(action)


def compact(meta, own_blocks, per, n_rel, r, fields, list_ref):
    src_bits, dst_bits, slot_bits, rel_bits, own_bits = fields
    rows, lanes = meta.shape
    live = meta >= 0
    src = meta & ((1 << src_bits) - 1)
    dst = lax.shift_right_logical(meta, src_bits) & ((1 << dst_bits) - 1)
    rel = lax.shift_right_logical(meta, src_bits + dst_bits) & ((1 << rel_bits) - 1)
    slot = lax.broadcasted_iota(jnp.int32, meta.shape, 0) * lanes + lax.broadcasted_iota(jnp.int32, meta.shape, 1)
    base = slot | lax.shift_left(src, slot_bits) | lax.shift_left(rel, slot_bits + src_bits)
    top = slot_bits + src_bits + rel_bits
    base = base | (1 << (top + own_bits))
    bf = jnp.bfloat16
    hits = [live & (dst == own_block(d, per, n_rel, r)) for d in range(own_blocks)]
    flags = jnp.concatenate([jnp.where(hit, 1.0, 0.0) for hit in hits], axis=0).astype(bf)
    size = own_blocks * rows
    before = lax.broadcasted_iota(jnp.int32, (lanes, lanes), 0) < lax.broadcasted_iota(jnp.int32, (lanes, lanes), 1)
    in_row = jnp.dot(flags, jnp.where(before, 1.0, 0.0).astype(bf), preferred_element_type=jnp.float32)
    row_sum = jnp.dot(flags, jnp.ones((lanes, lanes), bf), preferred_element_type=jnp.float32).astype(bf)
    i = lax.broadcasted_iota(jnp.int32, (size, size), 0)
    j = lax.broadcasted_iota(jnp.int32, (size, size), 1)
    same = jnp.zeros((size, size), jnp.bool_)
    for d in range(own_blocks):
        lo, hi = d * rows, (d + 1) * rows
        same = same | ((i >= lo) & (i < hi) & (j >= lo) & (j < hi))
    ahead = jnp.where(same & (j < i), 1.0, 0.0).astype(bf)
    both = jnp.where(same, 1.0, 0.0).astype(bf)
    rows_before = jnp.dot(ahead, row_sum, preferred_element_type=jnp.float32)
    totals = jnp.dot(both, row_sum, preferred_element_type=jnp.float32)
    rank = jnp.full(meta.shape, -1.0, jnp.float32)
    entry = base
    start = jnp.zeros(meta.shape, jnp.float32)
    for d in range(own_blocks):
        part = slice(d * rows, (d + 1) * rows)
        place = start + rows_before[part] + in_row[part]
        rank = jnp.where(hits[d], place, rank)
        entry = jnp.where(hits[d], base | (d << top), entry)
        start = start + jnp.floor((totals[part] + (GROUP - 1)) * (1.0 / GROUP)) * GROUP
    pieces = [(lax.shift_right_logical(entry, 8 * q) & 255).astype(jnp.float32) for q in range(4)]
    row_entries = []
    for a in range(rows):
        parts = [piece[a : a + 1] for piece in pieces] + [jnp.zeros((4, lanes), jnp.float32)]
        row_entries.append(jnp.concatenate(parts, axis=0).astype(bf))
    places = lax.broadcasted_iota(jnp.int32, (lanes, lanes), 0).astype(jnp.float32)
    for k in range(list_ref.shape[0] - 1):
        ids = places + float(k * lanes)
        found = jnp.zeros((8, lanes), jnp.float32)
        for a in range(rows):
            hot = jnp.where(ids == rank[a : a + 1], 1.0, 0.0).astype(bf)
            found = found + lax.dot_general(
                row_entries[a], hot, (((1,), (1,)), ((), ())), preferred_element_type=jnp.float32
            )
        whole = found.astype(jnp.int32)
        line = whole[0:1]
        for q in range(1, 4):
            line = line | lax.shift_left(whole[q : q + 1], 8 * q)
        list_ref[k : k + 1] = line
    groups = (start[0:1] * (1.0 / GROUP)).astype(jnp.int32)
    list_ref[list_ref.shape[0] - 1 :] = groups


def pack(src, dst, count, perm, fields, lanes):
    positions, tcap = src.shape
    i = lax.broadcasted_iota(jnp.int32, (positions, positions), 0)
    j = lax.broadcasted_iota(jnp.int32, (positions, positions), 1)

    def upright(row):
        return jnp.sum(jnp.where(i == j, row.astype(jnp.float32), 0.0), axis=1, keepdims=True).astype(jnp.int32)

    word = src | lax.shift_left(dst, fields[0]) | lax.shift_left(upright(perm), fields[0] + fields[1])
    slot = lax.broadcasted_iota(jnp.int32, src.shape, 1)
    word = jnp.where(slot < upright(count), word, -1)
    each = lanes // tcap
    rows = [
        jnp.concatenate([word[a + b : a + b + 1] for b in range(each)], axis=1) for a in range(0, positions, each)
    ]
    rows.append(jnp.full((8 - len(rows), lanes), -1, jnp.int32))
    return jnp.concatenate(rows, axis=0).reshape(1, 8, lanes)


def prepare_kernel(n_rel, n_node, n_head, fields, *refs):
    (small, feat_ref, wk_ref, wv_ref, wq_ref, msg_ref, bits_ref), refs = (
        (refs[:5],) + refs[5:11],
        refs[11:],
    )
    (kv_all, qt_ref, msg_out, bits_all, list_ref) = refs[:5]
    (x_v, wk_v, wv_v, wq_v, msg_v, meta_all), refs = refs[5:11], refs[11:]
    (types_ref, src_v, dst_v, count_v, perm_v), refs = refs[:5], refs[5:]
    (local, z_send, z_recv, v_send, y_send, y_recv, d_send, d_recv, m_send, m_recv, x_send, x_recv, f_send, f_recv) = refs
    blocks = types_ref.shape[0]
    block = types_ref.shape[1]
    cols = wk_v.shape[2]
    kinds = wk_v.shape[0]
    slots = bits_ref.shape[0]
    share = slots // n_head
    own_blocks = qt_ref.shape[0]
    per = own_blocks // n_head
    chunks = blocks // CHUNK
    rows = CHUNK * block
    relations, heads, size = msg_v.shape[:3]
    r = lax.axis_index("rel")
    n = lax.axis_index("node")
    h = lax.axis_index("head")
    sibling = h + 1 - 2 * lax.rem(h, 2)
    parity = lax.rem(r, 2)
    partner = r + 1 - 2 * parity
    pairs = list(range(2, n_head, 2))
    bf = jnp.bfloat16

    def fetch(src, dst, index):
        copy = pltpu.make_async_copy(src, dst, local.at[index])
        copy.start()
        return copy

    small_v = (types_ref, src_v, dst_v, count_v, perm_v)
    got_small = [fetch(a, b, 8 + chunks + i) for i, (a, b) in enumerate(zip(small, small_v))]
    own_bits = fetch(bits_ref, bits_all.at[pl.ds(pl.multiple_of(r * slots, slots), slots)], 0)
    got_w = [fetch(wk_ref, wk_v, 1), fetch(wv_ref, wv_v, 2)]
    got_x = []
    for c in range(chunks):
        got_x.append(fetch(feat_ref.at[pl.ds(c * rows, rows)], x_v.at[pl.ds(c * rows, rows)], 8 + c))
    got_q = fetch(wq_ref, wq_v, 3)
    got_rel = fetch(msg_ref, msg_v, 4)

    barrier = pltpu.get_barrier_semaphore()
    for t in range(1, n_rel):
        pl.semaphore_signal(barrier, inc=1, device_id={"rel": lax.rem(r + t, n_rel)})
    for t in range(1, n_node):
        pl.semaphore_signal(barrier, inc=1, device_id={"node": lax.rem(n + t, n_node)})
    for t in pairs:
        pl.semaphore_signal(barrier, inc=1, device_id={"head": lax.rem(h + t, n_head)})
    pl.semaphore_signal(barrier, inc=1, device_id={"head": sibling})
    for copy in got_small:
        copy.wait()
    meta_all[pl.ds(r, 1)] = pack(src_v[...], dst_v[...], count_v[...], perm_v[...], fields, block)
    pl.semaphore_wait(barrier, n_rel - 1 + n_node - 1 + len(pairs) + 1)

    started, guarded = [], []

    def send(src, dst, send_sem, recv_sem, target):
        copy = pltpu.make_async_remote_copy(
            src_ref=src, dst_ref=dst, send_sem=send_sem, recv_sem=recv_sem, device_id=target
        )
        copy.start()
        started.append(copy)
        return copy

    steps, inner = along_rel(n_rel, r)
    relayed = 3 if inner is not None else None
    part_rows = share // PIECES

    def bit_rows(rel, head, piece):
        first = rel * slots + head * share + piece * part_rows
        return bits_all.at[pl.ds(pl.multiple_of(first, part_rows), part_rows)]

    def send_bits(rel, head, piece, sems, index, target, condition=None):
        rows = bit_rows(rel, head, piece)
        copy = pltpu.make_async_remote_copy(
            src_ref=rows,
            dst_ref=rows,
            send_sem=sems[0].at[index],
            recv_sem=sems[1].at[index],
            device_id=target,
        )
        only_if(condition, copy.start)
        guarded.append((condition, copy))
        return copy

    own_bits.wait()
    metas, zs = [], {}
    for u, (peer, _) in steps.items():
        metas.append(send(meta_all.at[r], meta_all.at[r], m_send.at[u], m_recv.at[u], {"rel": peer}))
    for u, (peer, _) in steps.items():
        for q in range(PIECES):
            condition = inner if u == relayed else None
            zs[u, q] = send_bits(r, h, q, (z_send, z_recv), (u, q), {"rel": peer}, condition)

    for copy in got_w:
        copy.wait()
    xs, halves = [], []
    for c in range(chunks):
        got_x[c].wait()
        x = x_v[c * rows : (c + 1) * rows]
        masks = [column(types_ref[c * CHUNK + b : c * CHUNK + b + 1, :]) for b in range(CHUNK)]
        totals = [None] * CHUNK
        for kind in range(kinds):
            both = jnp.concatenate([wk_v[kind], wv_v[kind]], axis=1)
            out = jnp.dot(x, both, preferred_element_type=jnp.float32)
            for b in range(CHUNK):
                piece = out[b * block : (b + 1) * block]
                pair = (piece[:, :cols], piece[:, cols:])
                if totals[b] is None:
                    totals[b] = pair
                else:
                    hit = masks[b] == float(kind)
                    totals[b] = tuple(jnp.where(hit, new, old) for new, old in zip(pair, totals[b]))
        first = n * blocks + c * CHUNK
        for b in range(CHUNK):
            kv_all[0, first + b] = totals[b][0].astype(bf)
            kv_all[1, first + b] = totals[b][1].T.astype(bf)
        for t in range(1, n_node):
            target = {"node": lax.rem(n + t, n_node)}
            if c < SPLIT:
                part = kv_all.at[parity, pl.ds(first, CHUNK)]
                halves.append((t, c, send(part, part, x_send.at[t, c, 0], x_recv.at[t, c, 0], target)))
            else:
                for which in range(2):
                    part = kv_all.at[which, pl.ds(first, CHUNK)]
                    xs.append(send(part, part, x_send.at[t, c, which], x_recv.at[t, c, which], target))

    def forward(chunk):
        for t, c, copy in halves:
            if c == chunk:
                copy.wait_recv()
                first = lax.rem(n + n_node - t, n_node) * blocks + c * CHUNK
                part = kv_all.at[parity, pl.ds(first, CHUNK)]
                xs.append(send(part, part, f_send.at[t, c], f_recv.at[t, c], {"rel": partner}))

    got_q.wait()
    wide = jnp.concatenate([wq_v[kind] for kind in range(kinds)], axis=1)
    mine = [own_block(d, per, n_rel, r) for d in range(own_blocks)]
    x = jnp.concatenate([x_v[pl.ds(pl.multiple_of(b * block, block), block)] for b in mine], axis=0)
    out = jnp.dot(x, wide, preferred_element_type=jnp.float32)
    for d in range(own_blocks):
        mask = column(types_ref[pl.ds(mine[d], 1), :])
        piece = out[d * block : (d + 1) * block]
        total = piece[:, :cols]
        for kind in range(1, kinds):
            total = jnp.where(mask == float(kind), piece[:, kind * cols : (kind + 1) * cols], total)
        qt_ref[d] = total.T.astype(bf)

    got_rel.wait()
    unit = lax.broadcasted_iota(jnp.int32, (size, size), 0) == lax.broadcasted_iota(jnp.int32, (size, size), 1)
    unit = jnp.where(unit, 1.0, 0.0).astype(bf)
    owner = lax.broadcasted_iota(jnp.int32, (size, cols), 1) // size

    def relation(index, carry):
        flat = msg_v[pl.ds(index * BATCH, BATCH)].reshape(BATCH * cols, size)
        turned = lax.dot_general(unit, flat, (((1,), (1,)), ((), ())), preferred_element_type=jnp.float32)
        for i in range(BATCH):
            both = turned[:, i * cols : (i + 1) * cols]
            for k in range(heads):
                part = jnp.where(owner == k, both, 0.0).astype(bf)
                msg_out[index * BATCH + i, k * size : (k + 1) * size] = part
        return carry

    ys, ds = [], []
    for turn, (u, (_, source)) in enumerate(steps.items()):
        for q in range(PIECES):
            zs[u, q].wait_recv()
            if relayed and u == 2:
                send_bits(source, h, q, (v_send, z_recv), (relayed, q), {"rel": steps[1][0]}, inner)
            for i, t in enumerate(pairs):
                target = {"head": lax.rem(h + t, n_head)}
                ys.append((source, u, q, t, send_bits(source, h, q, (y_send, y_recv), (u, q, i), target)))
            ds.append(send_bits(source, h, q, (d_send, d_recv), (u, q, 0), {"head": sibling}))
        if turn < SPLIT:
            forward(turn)

    lax.fori_loop(0, relations // BATCH, relation, 0)
    for copy in metas:
        copy.wait_recv()
    used = slots // block
    meta = jnp.concatenate([meta_all[s, :used] for s in range(n_rel)], axis=0)
    compact(meta, own_blocks, per, n_rel, r, fields, list_ref)

    for c in range(n_rel - 1, SPLIT):
        forward(c)
    for source, u, q, t, copy in ys:
        copy.wait_recv()
        head = lax.rem(h + n_head - t, n_head)
        ds.append(send_bits(source, head, q, (d_send, d_recv), (u, q, 1 + pairs.index(t)), {"head": sibling}))
    for copy in ds:
        copy.wait_recv()
    for copy in xs:
        copy.wait_recv()
    for copy in started:
        copy.wait_send()
    for condition, copy in guarded:
        only_if(condition, copy.wait_send)


def tile_kernel(heads, factor, fields, list_ref, prior_ref, qt_ref, kv_ref, bits_ref, att_ref, msg_ref, *refs):
    acc_ref, top_ref = refs[:2]
    lefts, rights, scoress, peaks = refs[2:4], refs[4:6], refs[6:8], refs[8:10]
    src_bits, _, slot_bits, rel_bits, own_bits = fields
    own_blocks, cols, block = qt_ref.shape
    size = cols // heads
    words = bits_ref.shape[1]
    tall = acc_ref.shape[2]
    groups = list_ref[list_ref.shape[0] - 1, 0]

    acc_ref[...] = jnp.zeros_like(acc_ref)
    top_ref[...] = jnp.full_like(top_ref, FLOOR)
    for right in rights:
        right[...] = jnp.zeros_like(right)
    row = lax.broadcasted_iota(jnp.int32, (tall - size, GROUP * block), 0)
    ones = jnp.where(row == 0, 1.0, 0.0).astype(jnp.bfloat16)
    for left in lefts:
        for k in range(heads):
            left[k, size:] = ones
    bit_of = lax.shift_left(jnp.int32(1), lax.broadcasted_iota(jnp.int32, (32, block), 0))

    def entries(group):
        line = lax.shift_right_logical(group * GROUP, 7)
        start = (group * GROUP) & 127
        found = []
        for u in range(GROUP):
            value = list_ref[line, start + u]
            slot = value & ((1 << slot_bits) - 1)
            rest = lax.shift_right_logical(value, slot_bits)
            src = rest & ((1 << src_bits) - 1)
            rest = lax.shift_right_logical(rest, src_bits)
            rel = rest & ((1 << rel_bits) - 1)
            rest = lax.shift_right_logical(rest, rel_bits)
            dst = rest & ((1 << own_bits) - 1)
            valid = -lax.shift_right_logical(rest, own_bits)
            found.append((slot, src, rel, dst, valid))
        return found

    def turned_of(picks):
        dst = picks[0][3]
        found = []
        for k in range(heads):
            stack = jnp.concatenate([att_ref[rel, k] for _, _, rel, _, _ in picks], axis=0)
            query = qt_ref[dst, k * size : (k + 1) * size]
            found.append(jnp.dot(stack, query, preferred_element_type=jnp.float32))
        return found

    def keep_turned(picks, turned, right):
        for u, (_, _, rel, _, _) in enumerate(picks):
            for k in range(heads):
                scaled = turned[k][u * size : (u + 1) * size] * (prior_ref[k, rel] * factor)
                right[u, k * size : (k + 1) * size, k * block : (k + 1) * block] = scaled.astype(jnp.bfloat16)

    def messages_of(picks):
        return [jnp.dot(msg_ref[rel], kv_ref[1, src], preferred_element_type=jnp.float32) for _, src, rel, _, _ in picks]

    def keep_messages(messages, left):
        for u, message in enumerate(messages):
            for k in range(heads):
                lo = u * block
                left[k, :size, lo : lo + block] = message[k * size : (k + 1) * size].astype(jnp.bfloat16)

    def scores_of(picks, right):
        return [
            jnp.dot(kv_ref[0, src], right[u], preferred_element_type=jnp.float32)
            for u, (_, src, _, _, _) in enumerate(picks)
        ]

    def keep_scores(picks, found, scores, peak):
        best = [None] * heads
        for u, (slot, _, _, _, valid) in enumerate(picks):
            tile_words = bits_ref[slot] & valid
            edges = jnp.concatenate([(tile_words[w : w + 1] & bit_of) != 0 for w in range(words)], axis=0)
            for k in range(heads):
                masked = jnp.where(edges, found[u][:, k * block : (k + 1) * block], NEG)
                scores[u * heads + k] = masked
                top = jnp.max(masked.reshape(block // 8, 8, block), axis=0)
                best[k] = top if best[k] is None else jnp.maximum(best[k], top)
        for k in range(heads):
            peak[k : k + 1] = jnp.max(best[k], axis=0, keepdims=True)

    def gather(dst, left, scores, peak):
        outs = []
        for k in range(heads):
            old = top_ref[dst, k : k + 1]
            new = jnp.maximum(old, peak[k : k + 1])
            top_ref[dst, k : k + 1] = new
            weights = [jnp.exp(scores[u * heads + k] - new).astype(jnp.bfloat16) for u in range(GROUP)]
            out = jnp.dot(left[k], jnp.concatenate(weights, axis=0), preferred_element_type=jnp.float32)
            outs.append((jnp.exp(old - new), out))
        for k, (keep, out) in enumerate(outs):
            acc_ref[dst, k] = acc_ref[dst, k] * keep + out

    def visit(pair, carry):
        picks = [entries(pair * 2 + i) for i in range(4)]
        for i in range(2):
            now, soon, later = picks[i : i + 3]
            this, other = i, 1 - i
            keep_messages(messages_of(soon), lefts[other])
            found = scores_of(soon, rights[other])
            keep_turned(later, turned_of(later), rights[this])
            gather(now[0][3], lefts[this], scoress[this], peaks[this])
            keep_scores(soon, found, scoress[other], peaks[other])
        return carry

    first = entries(0)
    keep_turned(first, turned_of(first), rights[0])
    keep_scores(first, scores_of(first, rights[0]), scoress[0], peaks[0])
    keep_messages(messages_of(first), lefts[0])
    first = entries(1)
    keep_turned(first, turned_of(first), rights[1])
    lax.fori_loop(0, lax.shift_right_logical(groups + 1, 1), visit, 0)


def finish_kernel(n_rel, n_head, heads, acc_ref, types_ref, skip_ref, feat_ref, *refs):
    outs_w, refs = refs[: n_head // 2], refs[n_head // 2 :]
    out_ref, hid_out, hid_got, resid, w_ref, send_sem, recv_sem, relay_sem, w_send, w_recv, local = refs
    own_blocks, _, _, block = acc_ref.shape
    kinds = w_ref.shape[1]
    cols = w_ref.shape[2]
    width = w_ref.shape[3]
    size = cols // heads
    per = own_blocks // n_head
    piece = per * block
    r = lax.axis_index("rel")
    h = lax.axis_index("head")
    span = n_rel * piece

    fetch = pltpu.make_async_copy(feat_ref.at[pl.ds(pl.multiple_of(h * span, span), span)], resid, local.at[0])
    fetch.start()
    loads = []
    for i, got in enumerate(outs_w):
        head = lax.rem(h + n_head - 2 * i, n_head)
        loads.append((head, pltpu.make_async_copy(got, w_ref.at[head], local.at[1 + i])))
        loads[-1][1].start()
    steps, inner = along_rel(n_rel, r)
    relayed = 3 if inner is not None else None
    steps[0] = (r, r)
    barrier = pltpu.get_barrier_semaphore()
    shifts = [(u, b) for u in steps for b in range(n_head) if u or b]
    for u, b in shifts:
        pl.semaphore_signal(barrier, inc=1, device_id={"rel": steps[u][0], "head": lax.rem(h + b, n_head)})

    def hidden_of(source):
        sides = []
        for k in range(heads):
            total = jnp.maximum(acc_ref[source, k, size : size + 1], 1.0)
            sides.append(acc_ref[source, k, :size] / total)
        agg = jnp.concatenate(sides, axis=0)
        inner = math.sqrt(2.0 / math.pi) * (agg + 0.044715 * (agg * agg * agg))
        hidden = agg * (0.5 * (1.0 + jnp.tanh(inner)))
        return hidden.T.astype(jnp.bfloat16)

    for b in range(n_head):
        head = lax.rem(h + b, n_head)
        for i in range(per):
            hid_out[b, i * block : (i + 1) * block] = hidden_of(head * per + i)
    pl.semaphore_wait(barrier, len(shifts))

    sends, guarded = {}, []

    def pass_on(source, u, b, sem, target, condition):
        copy = pltpu.make_async_remote_copy(
            src_ref=source,
            dst_ref=hid_got.at[u, b],
            send_sem=sem.at[u, b],
            recv_sem=recv_sem.at[u, b],
            device_id=target,
        )
        only_if(condition, copy.start)
        guarded.append((condition, copy))
        return copy

    for u, b in shifts:
        target = {"rel": steps[u][0], "head": lax.rem(h + b, n_head)}
        sends[u, b] = pass_on(hid_out.at[b], u, b, send_sem, target, inner if u == relayed else None)
    hid_got[0, 0] = hid_out[0]
    shared = []
    for i, (head, load) in enumerate(loads):
        load.wait()
        copy = pltpu.make_async_remote_copy(
            src_ref=w_ref.at[head],
            dst_ref=w_ref.at[head],
            send_sem=w_send.at[i],
            recv_sem=w_recv.at[i],
            device_id={"head": h + 1 - 2 * lax.rem(h, 2)},
        )
        copy.start()
        shared.append(copy)
    fetch.wait()
    for copy in shared:
        copy.wait_recv()
    order = [u for u in (2, 0, 1, 3) if u in steps] + [u for u in steps if u > 3]
    for u in order:
        source = steps[u][1]
        for b in range(n_head):
            if u or b:
                sends[u, b].wait_recv()
                if relayed and u == 2:
                    pass_on(hid_got.at[u, b], relayed, b, relay_sem, {"rel": steps[1][0]}, inner)
        parts = [hid_got[u, lax.rem(h + n_head - head, n_head)] for head in range(n_head)]
        hidden = jnp.concatenate(parts, axis=1)
        outs = []
        for kind in range(kinds):
            weights = jnp.concatenate([w_ref[head, kind] for head in range(n_head)], axis=0)
            outs.append(jnp.dot(hidden, weights, preferred_element_type=jnp.float32))
        for i in range(per):
            mask = column(types_ref[pl.ds((h * n_rel + source) * per + i, 1), :])
            masks = [mask == float(kind) for kind in range(kinds)]
            logit = jnp.full((block, block), skip_ref[0], jnp.float32)
            for kind in range(1, kinds):
                logit = jnp.where(masks[kind], skip_ref[kind], logit)
            gate = 1.0 / (1.0 + jnp.exp(-logit))
            rows = pl.ds(pl.multiple_of(source * piece + i * block, block), block)
            for w in range(width // block):
                lanes = slice(w * block, (w + 1) * block)
                total = outs[0][i * block : (i + 1) * block, lanes]
                for kind in range(1, kinds):
                    total = jnp.where(masks[kind], outs[kind][i * block : (i + 1) * block, lanes], total)
                old = resid[rows, lanes].astype(jnp.float32)
                out_ref[rows, lanes] = (gate * total + (1.0 - gate) * old).astype(jnp.bfloat16)
    for copy in shared:
        copy.wait_send()
    for condition, copy in guarded:
        only_if(condition, copy.wait_send)


def per_device(
    features,
    node_type,
    w_query,
    w_key,
    w_value,
    rel_att,
    rel_msg,
    rel_prior,
    w_out,
    skip,
    rel_perm,
    tile_src,
    tile_dst,
    tile_bits,
    tile_count,
):
    node_rows, width = features.shape
    n_rel = lax.axis_size("rel")
    n_node = lax.axis_size("node")
    n_head = lax.axis_size("head")
    relations, heads = rel_prior.shape
    cols = w_query.shape[2]
    kinds = w_query.shape[0]
    block = tile_bits.shape[2]
    words = tile_bits.shape[3]
    blocks = node_rows // block
    positions, tcap = tile_src.shape
    slots = positions * tcap
    factor = 1.0 / math.sqrt(cols // heads)
    own_blocks = blocks // n_rel
    all_slots = n_rel * slots
    bf = jnp.bfloat16
    fields = (
        bits_for(n_node * blocks),
        bits_for(blocks),
        bits_for(all_slots),
        bits_for(relations),
        bits_for(own_blocks),
    )

    bits = tile_bits.transpose(0, 1, 3, 2).reshape(slots, words, block)

    list_rows = -(-(all_slots + own_blocks * GROUP + 4 * GROUP) // block) + 1
    chunks = blocks // CHUNK
    half = max(n_head // 2 - 1, 1)
    dma = pltpu.SemaphoreType.DMA
    smem = pl.BlockSpec(memory_space=pltpu.SMEM)
    vmem = pl.BlockSpec(memory_space=pltpu.VMEM)
    hbm = pl.BlockSpec(memory_space=pltpu.HBM)
    shape = jax.ShapeDtypeStruct
    operands = (
        node_type.reshape(blocks, block),
        tile_src,
        tile_dst,
        tile_count.reshape(1, positions),
        rel_perm.reshape(1, positions),
        features,
        w_key,
        w_value,
        w_query,
        rel_msg,
        bits,
    )
    pairs_kv, query_t, msg, all_bits, listed = pl.pallas_call(
        functools.partial(prepare_kernel, n_rel, n_node, n_head, fields),
        in_specs=[hbm] * 11,
        out_specs=[vmem] * 5,
        out_shape=[
            shape((2, n_node * blocks, block, cols), bf),
            shape((own_blocks, cols, block), bf),
            shape((relations, cols, cols), bf),
            shape((all_slots, words, block), jnp.int32),
            shape((list_rows, block), jnp.int32),
        ],
        scratch_shapes=[
            pltpu.VMEM(features.shape, bf),
            pltpu.VMEM(w_key.shape, bf),
            pltpu.VMEM(w_value.shape, bf),
            pltpu.VMEM(w_query.shape, bf),
            pltpu.VMEM(rel_msg.shape, bf),
            pltpu.VMEM((n_rel, 8, block), jnp.int32),
            pltpu.VMEM((blocks, block), jnp.int32),
            pltpu.VMEM((positions, tcap), jnp.int32),
            pltpu.VMEM((positions, tcap), jnp.int32),
            pltpu.VMEM((1, positions), jnp.int32),
            pltpu.VMEM((1, positions), jnp.int32),
            dma((13 + chunks,)),
            dma((n_rel, PIECES)),
            dma((n_rel, PIECES)),
            dma((n_rel, PIECES)),
            dma((n_rel, PIECES, half)),
            dma((n_rel, PIECES, half)),
            dma((n_rel, PIECES, 1 + half)),
            dma((n_rel, PIECES, 1 + half)),
            dma((n_rel,)),
            dma((n_rel,)),
            dma((n_node, chunks, 2)),
            dma((n_node, chunks, 2)),
            dma((n_node, chunks)),
            dma((n_node, chunks)),
        ],
        compiler_params=pltpu.CompilerParams(collective_id=0, has_side_effects=True, vmem_limit_bytes=VMEM_BYTES),
        name="prepare",
    )(*[in_hbm(value) for value in operands])

    late_out, listed = lax.optimization_barrier((w_out, listed))
    gathered = [w_out]
    for shift in range(2, n_head, 2):
        pairs = [(i, (i + shift) % n_head) for i in range(n_head)]
        gathered.append(lax.ppermute(late_out, "head", pairs))
    tall = cols // heads + PAD_ROWS
    acc = pl.pallas_call(
        functools.partial(tile_kernel, heads, factor, fields),
        in_specs=[smem] * 2 + [vmem] * 5,
        out_specs=vmem,
        out_shape=shape((own_blocks, heads, tall, block), jnp.float32),
        scratch_shapes=[
            pltpu.VMEM((own_blocks, 8, block), jnp.float32),
            *[pltpu.VMEM((heads, tall, GROUP * block), bf)] * 2,
            *[pltpu.VMEM((GROUP, cols, heads * block), bf)] * 2,
            *[pltpu.VMEM((GROUP * heads, block, block), jnp.float32)] * 2,
            *[pltpu.VMEM((8, block), jnp.float32)] * 2,
        ],
        compiler_params=pltpu.CompilerParams(vmem_limit_bytes=VMEM_BYTES),
        name="tiles",
    )(listed, rel_prior.T, query_t, pairs_kv, all_bits, rel_att, msg)

    piece = own_blocks // n_head * block
    return pl.pallas_call(
        functools.partial(finish_kernel, n_rel, n_head, heads),
        in_specs=[vmem, vmem, smem, hbm, hbm] + [vmem] * (len(gathered) - 1),
        out_specs=vmem,
        out_shape=shape((n_rel * piece, width), bf),
        scratch_shapes=[
            pltpu.VMEM((n_head, piece, cols), bf),
            pltpu.VMEM((n_rel, n_head, piece, cols), bf),
            pltpu.VMEM((n_rel * piece, width), bf),
            pltpu.VMEM((n_head,) + w_out.shape, bf),
            dma((n_rel, n_head)),
            dma((n_rel, n_head)),
            dma((n_rel, n_head)),
            dma((n_head,)),
            dma((n_head,)),
            dma((1 + n_head,)),
        ],
        compiler_params=pltpu.CompilerParams(collective_id=1, has_side_effects=True, vmem_limit_bytes=VMEM_BYTES),
        name="finish",
    )(acc, node_type.reshape(blocks, block), skip, in_hbm(features), in_hbm(w_out), *gathered[1:])


def solution(mesh):
    in_specs = (
        P("node", None),
        P("node"),
        P(None, None, "head"),
        P(None, None, "head"),
        P(None, None, "head"),
        P(None, "head", None, None),
        P(None, "head", None, None),
        P(None, "head"),
        P(None, "head", None),
        P(),
        P("rel"),
        P("rel", "node"),
        P("rel", "node"),
        P("rel", "node", None, None),
        P("rel", "node"),
    )
    out_specs = P(("node", "head"), None)
    return jax.shard_map(
        per_device, mesh=mesh, in_specs=in_specs, out_specs=out_specs, check_vma=False
    )
```
